32 devices in a mesh: dom: 16 (over z, y, x), tm: 2 (over core).
Axes of the slice: x: 2, y: 2, z: 4, core: 2. Of those that a mesh axis runs over, the one named last changes fastest.
Arguments:
- sources: bfloat16 [256, 3, 16, 256], P('dom', None, 'tm'), may hold values from -6 to 6
- weights: bfloat16 [48, 16, 256, 256], P('dom', None, None, 'tm'), may hold values from -0.09375 to 0.09375
- intersect: int32 [48, 16], replicated, may hold values from 0 to 255, as said below
- block_row: int32 [256], replicated, may hold values from 0 to 255, as said below
- slot_tile: int32 [48], replicated, may hold values from 0 to 47, as said below
Outputs:
- acoustic_source: bfloat16 [48, 3, 16, 256], P('dom', None, 'tm')
- source_rate: bfloat16 [48, 3, 16, 256], P('dom', None, 'tm')
The draws below stay inside these ranges and needn't reach their ends.
Inputs may be any that keep to these rules, and one draw needn't show every extreme that they name: `intersect`: over the 48 links of the slots held by one index of dom, exactly 24 distinct source rows are named, each by exactly two links; no index of dom holds more than 2 of these rows, and some index holds exactly 2. `block_row`: A permutation of the block ids. `slot_tile`: A permutation of the tile ids.
All inputs are finite; a program needn't handle non-finite values.
Results may differ from the reference program's by a relative error of at most 0.007.
Values may be sent and summed in bfloat16 or wider, within the bound.
A program may use at most 64 MiB of HBM per device.

```python
import jax
import jax.numpy as jnp
from jax import lax

CELLS = 256
NODES = 256
COMP = 3
TS = 16
BLK_DEV = 16
TILE_DEV = 3
K = 16
NB = 256
NA = 48
POOL = 24


def link_layout(key):
    domain_count = NB // BLK_DEV
    per_owner = (POOL + domain_count - 1) // domain_count
    slot_count = domain_count * per_owner
    popular = jax.random.randint(jax.random.fold_in(key, 7), (domain_count,), 0, 4).astype(jnp.int32)
    owner_of = jnp.arange(slot_count, dtype=jnp.int32) // per_owner
    within = jnp.arange(slot_count, dtype=jnp.int32) % per_owner

    def device_links(device_key):
        score_key, offset_key, shuffle_key = jax.random.split(device_key, 3)
        jitter = jax.random.randint(score_key, (slot_count,), 0, 4096).astype(jnp.int32)
        scores = (popular[owner_of] * 4096 + jitter) * slot_count + jnp.arange(slot_count, dtype=jnp.int32)
        chosen = jnp.argsort(-scores)[:POOL]
        row_base = jax.random.randint(offset_key, (domain_count,), 0, BLK_DEV).astype(jnp.int32)
        chosen_owner = owner_of[chosen]
        rows_pool = chosen_owner * BLK_DEV + (row_base[chosen_owner] + within[chosen]) % BLK_DEV
        doubled = jnp.concatenate([rows_pool, rows_pool])
        shuffle = jax.random.permutation(shuffle_key, 2 * POOL)
        return doubled[shuffle].reshape(TILE_DEV, K)
    device_keys = jax.random.split(jax.random.fold_in(key, 3), domain_count)
    by_slot = jax.vmap(device_links)(device_keys).reshape(NA, K)
    block_row = jax.random.permutation(jax.random.fold_in(key, 11), NB).astype(jnp.int32)
    row_block = jnp.argsort(block_row).astype(jnp.int32)
    slot_tile = jax.random.permutation(jax.random.fold_in(key, 13), NA).astype(jnp.int32)
    tile_slot = jnp.argsort(slot_tile).astype(jnp.int32)
    intersect = row_block[by_slot][tile_slot]
    return (intersect.astype(jnp.int32), block_row, slot_tile)


def draw_intersect(key, part):
    return link_layout(key)[0]


def draw_block_row(key, part):
    return link_layout(key)[1]


def draw_slot_tile(key, part):
    return link_layout(key)[2]


def block_scale(key, extent, cuts, low, largest):
    gain, own = 1.0, jax.random.fold_in(key, 6)
    for axis_at, blocks in cuts:
        heights = jnp.exp(jax.random.uniform(jax.random.fold_in(own, axis_at), (blocks,), jnp.float32, low / len(cuts), largest / len(cuts)))
        gain = gain * jnp.repeat(heights, extent[axis_at] // blocks).reshape([-1 if axis == axis_at else 1 for axis in range(len(extent))])
    return gain


def noise(key, extent, deviation, limit, cuts=(), kind=jnp.bfloat16):
    values = deviation * jax.random.normal(key, extent, jnp.float32)
    if cuts:
        values = values * block_scale(key, extent, cuts, -0.22, 0.18)
    return jnp.clip(values, -limit, limit).astype(kind)


def setup_inputs(seed: int = 0) -> dict:
    key_list = jax.random.split(jax.random.key(seed), 6)
    return {
        "sources": noise(key_list[0], (NB, COMP, TS, CELLS), 1.0, 6.0, ((0, 16), (2, 2))),
        "weights": noise(key_list[1], (NA, K, CELLS, NODES), (K * CELLS) ** -0.5, 0.09375, ((0, 16), (3, 2))),
        "intersect": draw_intersect(jax.random.fold_in(key_list[5], 71), 0),
        "block_row": draw_block_row(jax.random.fold_in(key_list[5], 71), 0),
        "slot_tile": draw_slot_tile(jax.random.fold_in(key_list[5], 71), 0),
    }


def time_derivative(values):
    central = (values[:, 2:] - values[:, :-2]) * 0.5
    first_edge = values[:, 1:2] - values[:, 0:1]
    last_edge = values[:, -1:] - values[:, -2:-1]
    return jnp.concatenate([first_edge, central, last_edge], axis=1)


def reference(sources, weights, intersect, block_row, slot_tile):
    link_rows = jnp.take(block_row, jnp.take(intersect, slot_tile, axis=0), axis=0).astype(jnp.int32)

    def one_tile(inputs):
        tile_rows, tile_weights = inputs
        picked = jnp.take(sources, tile_rows, axis=0).astype(jnp.float32)
        combined = jnp.einsum("kpsc,kcn->psn", picked, tile_weights.astype(jnp.float32), precision=lax.Precision.HIGHEST)
        return combined.astype(jnp.bfloat16), time_derivative(combined).astype(jnp.bfloat16)

    acoustic_source, source_rate = lax.map(one_tile, (link_rows, weights))
    return acoustic_source, source_rate
```

```python
import functools

import jax
import jax.numpy as jnp
from jax import lax
from jax.experimental import pallas as pl
from jax.experimental.pallas import tpu as pltpu
from jax.sharding import PartitionSpec as P


BIG = 1 << 30
LANES = 128


def lookup(table, index):
    within, group = index & (LANES - 1), index >> 7
    outs = []
    for at in range(0, index.shape[1], LANES):
        value = jnp.zeros((index.shape[0], LANES), jnp.int32)
        for g in range(table.shape[1] // LANES):
            got = jnp.take_along_axis(
                table[:, g * LANES : (g + 1) * LANES],
                within[:, at : at + LANES],
                axis=1,
                mode="promise_in_bounds",
            )
            value = jnp.where(group[:, at : at + LANES] == g, got, value)
        outs.append(value)
    return outs[0] if len(outs) == 1 else jnp.concatenate(outs, axis=1)


def steps(count, body):
    if count <= 16:
        for i in range(count):
            body(i)
    else:
        def step(i, carry):
            body(i)
            return carry
        lax.fori_loop(0, count, step, 0)


def kernel(
    domains, per_owner,
    tile_hbm, row_hbm, cross_hbm, src_hbm, w_hbm, out_ref,
    tile_ref, row_ref, cross_ref, src_ref,
    wide_tile, wide_row, wide_cross, send_to, link_one, link_two,
    w_ref, pack, buf, acc, edge, beyond,
    in_sem, w_sem, send_sem, recv_sem, wsend_sem, wrecv_sem, edge_sem, flag_sem, near_sem,
):
    me = lax.axis_index("dom")
    core = lax.axis_index("tm")
    other = 1 - core
    links, width = w_ref.shape[1], w_ref.shape[3]
    blocks, comps, half, cells = src_ref.shape
    tiles = acc.shape[0]
    link_count = links // tiles
    count = comps * half
    mesh_type = pl.DeviceIdType.MESH
    mid, quarter = domains // 2, domains // 4
    upper = me // mid
    lower = 1 - upper
    plane = me // quarter
    inner = (plane + 1) // 2 % 2 * quarter
    even = (1 - plane % 2) * quarter

    def key(d):
        return (1 - d // mid) * (d % 2 + d // 2 % 2 + d // 4) * domains + d

    def wait_if(condition, sem, value):
        @pl.when(condition)
        def _():
            pl.semaphore_wait(sem, value)

    def source_of(i):
        if domains == 16:
            if i < quarter:
                return me ^ i
            if i < 2 * quarter:
                return me ^ (domains - 1 - (i - quarter)) ^ inner
            if i < 3 * quarter:
                return me ^ (mid - 1 - (i - 2 * quarter))
            return me ^ (domains - 1 - quarter - (i - 3 * quarter)) ^ inner
        return me ^ i

    inputs = [
        pltpu.make_async_copy(source, target, in_sem.at[i])
        for i, (source, target) in enumerate(
            (
                (tile_hbm, tile_ref),
                (cross_hbm, cross_ref),
                (row_hbm, row_ref),
                (src_hbm, src_ref),
            )
        )
    ]
    for load in inputs:
        load.start()

    barrier = pltpu.get_barrier_semaphore()
    pl.semaphore_signal(barrier, inc=1, device_id=(me, other), device_id_type=mesh_type)

    def greet(i):
        across, near = domains - 1 - i, upper * mid + i

        @pl.when(upper == 0)
        def _():
            pl.semaphore_signal(
                barrier, inc=1, device_id=(across, core), device_id_type=mesh_type
            )

        @pl.when(key(near) > key(me))
        def _():
            pl.semaphore_signal(
                barrier, inc=1, device_id=(near, core), device_id_type=mesh_type
            )

    steps(mid, greet)

    load_w = pltpu.make_async_copy(w_hbm, w_ref.at[core], w_sem)
    load_w.start()

    wide_tile[...] = jnp.zeros_like(wide_tile)
    wide_cross[...] = jnp.zeros_like(wide_cross)
    wide_row[...] = jnp.zeros_like(wide_row)

    def swap_to(part):
        return pltpu.make_async_remote_copy(
            src_ref=w_hbm,
            dst_ref=w_ref.at[part],
            send_sem=wsend_sem,
            recv_sem=wrecv_sem,
            device_id=(me, other),
            device_id_type=mesh_type,
        )

    swap = swap_to(core)
    before = sum((key(upper * mid + i) < key(me)).astype(jnp.int32) for i in range(mid))

    def announce(i):
        near = upper * mid + i

        @pl.when(key(near) < key(me))
        def _():
            pl.semaphore_signal(near_sem, inc=1, device_id=(near, core), device_id_type=mesh_type)

        @pl.when(upper == 1)
        def _():
            pl.semaphore_signal(
                flag_sem.at[me % mid], inc=1, device_id=(i, core), device_id_type=mesh_type
            )

    @pl.when(upper == 0)
    def _():
        pl.semaphore_wait(barrier, 1 + before)
        steps(mid, announce)
        swap.start()

    for load in inputs[:3]:
        load.wait()
    wide_tile[:, : tile_ref.shape[1]] = jnp.broadcast_to(
        tile_ref[...], (link_count, tile_ref.shape[1])
    )
    wide_cross[:, : cross_ref.shape[1]] = cross_ref[...]
    wide_row[:, : row_ref.shape[1]] = jnp.broadcast_to(
        row_ref[...], (link_count, row_ref.shape[1])
    )
    owners = -(-domains // LANES) * LANES
    around = lax.broadcasted_iota(jnp.int32, (1, owners), 1)
    lane = lax.broadcasted_iota(jnp.int32, (link_count, owners), 1)
    named = lookup(wide_row[...], wide_cross[...])
    rows = []
    for t in range(tiles):
        slot = jnp.minimum(lane * tiles + t, tile_ref.shape[1] - 1)
        rows.append(lookup(named, lookup(wide_tile[...], slot)))

    base = me * blocks
    locals_ = [
        jnp.where((row >= base) & (row < base + blocks), row - base, BIG) for row in rows
    ]
    last = jnp.full((1, owners), -1, jnp.int32)
    for j in range(per_owner):
        left = [jnp.where(at > last, at, BIG) for at in locals_]
        last = jnp.min(functools.reduce(jnp.minimum, left), axis=0, keepdims=True)
        index = jnp.minimum(last, blocks - 1)
        for d in range(domains):
            send_to[d * per_owner + j] = index[0, d]

    def fill(d):
        for j in range(per_owner):
            pack[d, j] = src_ref[send_to[d * per_owner + j]]

    inputs[3].wait()
    steps(domains, fill)
    for j in range(per_owner):
        buf[me * per_owner + j] = src_ref[send_to[me * per_owner + j]]

    def exchange(to):
        return pltpu.make_async_remote_copy(
            src_ref=pack.at[to],
            dst_ref=buf.at[pl.ds(me * per_owner, per_owner)],
            send_sem=send_sem,
            recv_sem=recv_sem.at[me],
            device_id=(to, core),
            device_id_type=mesh_type,
        )

    def first(i):
        to = me ^ (domains - 1 - i) ^ even ^ (lower * (quarter - 1))
        wait_if(upper == 0, flag_sem.at[to % mid], 1)
        exchange(to).start()

    def second(i):
        to = me ^ (mid + quarter - 1 - i) ^ even
        wait_if(upper == 0, flag_sem.at[to % mid], 1)
        exchange(to).start()

    @pl.when(upper == 1)
    def _():
        pl.semaphore_wait(barrier, mid + 1 + before)
        steps(mid, announce)
        steps(quarter, first)
        steps(quarter, second)
        swap.start()

    wait_if(before < mid - 1, near_sem, mid - 1 - before)
    steps(mid - 1, lambda i: exchange(me ^ (mid - 1 - i)).start())

    @pl.when(upper == 0)
    def _():
        steps(quarter, first)
        steps(quarter, second)

    link = lax.broadcasted_iota(jnp.int32, (link_count, owners), 0)
    mine = []
    for t in range(tiles):
        column = jnp.sum(jnp.where(lane == me, rows[t], 0), axis=1, keepdims=True)
        at = column - around * blocks
        mine.append(jnp.where((at >= 0) & (at < blocks), at, BIG))
    last = jnp.full((1, owners), -1, jnp.int32)
    for j in range(per_owner):
        least = [jnp.where(at > last, at, BIG) for at in mine]
        last = jnp.min(functools.reduce(jnp.minimum, least), axis=0, keepdims=True)
        one = jnp.full((link_count, owners), BIG, jnp.int32)
        two = jnp.full((link_count, owners), -1, jnp.int32)
        for t in range(tiles):
            hit = (mine[t] == last) & (last < BIG)
            one = jnp.minimum(one, jnp.where(hit, link + t * link_count, BIG))
            two = jnp.maximum(two, jnp.where(hit, link + t * link_count, -1))
        one = jnp.min(one, axis=0, keepdims=True)
        two = jnp.max(two, axis=0, keepdims=True)
        for i in range(domains):
            link_one[i * per_owner + j] = one[0, i]
            link_two[i * per_owner + j] = two[0, i]

    acc[...] = jnp.zeros_like(acc)

    def product(i):
        frm = source_of(i)
        for j in range(per_owner):
            rows_here = buf[frm * per_owner + j].astype(jnp.float32)
            lhs = rows_here.reshape(count, cells).astype(jnp.bfloat16)
            one = link_one[frm * per_owner + j]
            two = link_two[frm * per_owner + j]
            at_one, at_two = jnp.minimum(one, links - 1), jnp.maximum(two, 0)
            quad = jnp.concatenate(
                [w_ref[0, at_one], w_ref[1, at_one], w_ref[0, at_two], w_ref[1, at_two]], axis=1
            )
            both = jnp.dot(lhs, quad, preferred_element_type=jnp.float32)
            for t in range(tiles):
                first, end = t * link_count, (t + 1) * link_count
                acc[t] += jnp.where(
                    (one >= first) & (one < end), both[:, : 2 * width], 0.0
                ) + jnp.where((two >= first) & (two < end), both[:, 2 * width :], 0.0)

    def arrive(i):
        frm = source_of(i)
        pltpu.make_async_remote_copy(
            src_ref=pack.at[0],
            dst_ref=buf.at[pl.ds(frm * per_owner, per_owner)],
            send_sem=send_sem,
            recv_sem=recv_sem.at[frm],
            device_id=(frm, core),
            device_id_type=mesh_type,
        ).wait_recv()

    load_w.wait()
    swap_to(other).wait_recv()

    product(0)

    def take(i):
        arrive(i + 1)
        product(i + 1)

    steps(domains - 1, take)

    total = acc[...].reshape(tiles, comps, half, 2 * width)
    edge[...] = jnp.where(core == 0, total[:, :, half - 1], total[:, :, 0])
    halo = pltpu.make_async_remote_copy(
        src_ref=edge,
        dst_ref=beyond,
        send_sem=edge_sem.at[0],
        recv_sem=edge_sem.at[1],
        device_id=(me, other),
        device_id_type=mesh_type,
    )
    out_ref[0] = total.astype(jnp.bfloat16)

    sent = pack.at[pl.ds(0, domains - 1)]
    pltpu.make_async_remote_copy(
        src_ref=sent,
        dst_ref=sent,
        send_sem=send_sem,
        recv_sem=recv_sem.at[me],
        device_id=(me, other),
        device_id_type=mesh_type,
    ).wait_send()
    swap.wait_send()
    halo.start()
    halo.wait()
    sample = lax.broadcasted_iota(jnp.int32, (half, 2 * width), 0)
    for t in range(tiles):
        for p in range(comps):
            now = total[t, p]
            outer = jnp.broadcast_to(beyond[t, pl.ds(p, 1)], now.shape)
            later = pltpu.roll(now, half - 1, 0)
            prior = pltpu.roll(now, 1, 0)
            later = jnp.where((sample == half - 1) & (core == 0), outer, later)
            prior = jnp.where((sample == 0) & (core == 1), outer, prior)
            rate = jnp.where(
                (sample == 0) & (core == 0),
                later - now,
                jnp.where(
                    (sample == half - 1) & (core == 1), now - prior, (later - prior) * 0.5
                ),
            )
            out_ref[1, t, p] = rate.astype(jnp.bfloat16)


def deliver(both_ref, source_ref, rate_ref, sem):
    copies = [
        pltpu.make_async_copy(both_ref.at[i], out, sem.at[i])
        for i, out in enumerate((source_ref, rate_ref))
    ]
    for copy in copies:
        copy.start()
    for copy in copies:
        copy.wait()


def shards(sources, weights, intersect, block_row, slot_tile):
    domains = lax.axis_size("dom")
    tiles, link_count, cells, width = weights.shape
    blocks, comps, half, _ = sources.shape
    links = tiles * link_count
    pool = links // 2
    per_owner = (pool + domains - 1) // domains
    vmem, smem = pltpu.VMEM, pltpu.SMEM
    shape = (tiles, comps, half, 2 * width)
    out = jax.ShapeDtypeStruct(shape, jnp.bfloat16)
    block = (comps, half, cells)
    dma, regular = pltpu.SemaphoreType.DMA, pltpu.SemaphoreType.REGULAR
    in_vmem = pl.BlockSpec(memory_space=vmem)
    anywhere = pl.BlockSpec(memory_space=pl.ANY)

    def wide(n):
        return vmem((link_count, -(-n // LANES) * LANES), jnp.int32)

    both = pl.pallas_call(
        functools.partial(kernel, domains, per_owner),
        out_shape=vmem((2,) + shape, jnp.bfloat16),
        in_specs=[anywhere] * 5,
        out_specs=in_vmem,
        scratch_shapes=[
            vmem((1, slot_tile.shape[0]), jnp.int32),
            vmem((1, block_row.shape[0]), jnp.int32),
            vmem((link_count, intersect.shape[0]), jnp.int32),
            vmem(sources.shape, jnp.bfloat16),
            wide(slot_tile.shape[0]),
            wide(block_row.shape[0]),
            wide(intersect.shape[0]),
            smem((domains * per_owner,), jnp.int32),
            smem((domains * per_owner,), jnp.int32),
            smem((domains * per_owner,), jnp.int32),
            vmem((2, links, cells, width), jnp.bfloat16),
            vmem((domains, per_owner) + block, jnp.bfloat16),
            vmem((domains * per_owner,) + block, jnp.bfloat16),
            vmem((tiles, comps * half, 2 * width), jnp.float32),
            vmem((tiles, comps, 2 * width), jnp.float32),
            vmem((tiles, comps, 2 * width), jnp.float32),
            dma((4,)),
            dma,
            dma,
            dma((domains,)),
            dma,
            dma,
            dma((2,)),
            regular((domains // 2,)),
            regular,
        ],
        compiler_params=pltpu.CompilerParams(collective_id=0, has_side_effects=True),
        cost_estimate=pl.CostEstimate(
            flops=4 * comps * half * weights.size,
            bytes_accessed=2 * weights.size,
            transcendentals=0,
        ),
    )(
        slot_tile.reshape(1, -1),
        block_row.reshape(1, -1),
        intersect.T,
        sources,
        weights.reshape(links, cells, width),
    )
    return pl.pallas_call(
        deliver,
        out_shape=(out, out),
        in_specs=[in_vmem],
        out_specs=(anywhere, anywhere),
        scratch_shapes=[dma((2,))],
    )(pltpu.with_memory_space_constraint(both, vmem))


def solution(mesh):
    return jax.shard_map(
        shards,
        mesh=mesh,
        in_specs=(P("dom", None, "tm", None), P("dom", None, None, "tm"), P(), P(), P()),
        out_specs=(P("dom", None, "tm", None), P("dom", None, "tm", None)),
        check_vma=False,
    )
```

```python
import functools

import jax
import jax.numpy as jnp
from jax import lax
from jax.experimental import pallas as pl
from jax.experimental.pallas import tpu as pltpu
from jax.sharding import PartitionSpec as P


BIG = 1 << 30
LANES = 128


def lookup(table, index):
    within, group = index & (LANES - 1), index >> 7
    outs = []
    for at in range(0, index.shape[1], LANES):
        value = jnp.zeros((index.shape[0], LANES), jnp.int32)
        for g in range(table.shape[1] // LANES):
            got = jnp.take_along_axis(
                table[:, g * LANES : (g + 1) * LANES],
                within[:, at : at + LANES],
                axis=1,
                mode="promise_in_bounds",
            )
            value = jnp.where(group[:, at : at + LANES] == g, got, value)
        outs.append(value)
    return outs[0] if len(outs) == 1 else jnp.concatenate(outs, axis=1)


def steps(count, body):
    if count <= 16:
        for i in range(count):
            body(i)
    else:
        def step(i, carry):
            body(i)
            return carry
        lax.fori_loop(0, count, step, 0)


def kernel(
    domains, per_owner,
    tile_hbm, row_hbm, cross_hbm, src_hbm, w_hbm, out_ref,
    tile_ref, row_ref, cross_ref, src_ref,
    wide_tile, wide_row, wide_cross, send_to, link_one, link_two,
    w_ref, pack, buf, acc, edge, beyond, twin_ref, rim_acc,
    in_sem, w_sem, send_sem, recv_sem, wsend_sem, wrecv_sem, edge_sem, flag_sem, near_sem,
    twin_sem,
):
    me = lax.axis_index("dom")
    core = lax.axis_index("tm")
    other = 1 - core
    links, width = w_ref.shape[1], w_ref.shape[3]
    blocks, comps, half, cells = src_ref.shape
    tiles = acc.shape[0]
    link_count = links // tiles
    count = comps * half
    full = per_owner * comps
    planes = full + 1
    mesh_type = pl.DeviceIdType.MESH
    mid, quarter = domains // 2, domains // 4
    upper = me // mid
    lower = 1 - upper
    plane = me // quarter
    inner = (plane + 1) // 2 % 2 * quarter
    even = (1 - plane % 2) * quarter

    def key(d):
        return (1 - d // mid) * (d % 2 + d // 2 % 2 + d // 4) * domains + d

    def wait_if(condition, sem, value):
        @pl.when(condition)
        def _():
            pl.semaphore_wait(sem, value)

    near_from = inner // quarter

    def mailbox(offset):
        return 2 + near_from * (1 + offset)

    inputs = [
        pltpu.make_async_copy(source, target, in_sem.at[i])
        for i, (source, target) in enumerate(
            (
                (tile_hbm, tile_ref),
                (cross_hbm, cross_ref),
                (row_hbm, row_ref),
                (src_hbm, src_ref),
            )
        )
    ]
    for load in inputs:
        load.start()

    barrier = pltpu.get_barrier_semaphore()
    pl.semaphore_signal(barrier, inc=1, device_id=(me, other), device_id_type=mesh_type)

    def greet(i):
        across, near = domains - 1 - i, upper * mid + i

        @pl.when(upper == 0)
        def _():
            pl.semaphore_signal(
                barrier, inc=1, device_id=(across, core), device_id_type=mesh_type
            )

        @pl.when(key(near) > key(me))
        def _():
            pl.semaphore_signal(
                barrier, inc=1, device_id=(near, core), device_id_type=mesh_type
            )

    steps(mid, greet)

    load_w = pltpu.make_async_copy(w_hbm, w_ref.at[core], w_sem)
    load_w.start()

    wide_tile[...] = jnp.zeros_like(wide_tile)
    wide_cross[...] = jnp.zeros_like(wide_cross)
    wide_row[...] = jnp.zeros_like(wide_row)

    def swap_to(part):
        return pltpu.make_async_remote_copy(
            src_ref=w_hbm,
            dst_ref=w_ref.at[part],
            send_sem=wsend_sem,
            recv_sem=wrecv_sem,
            device_id=(me, other),
            device_id_type=mesh_type,
        )

    swap = swap_to(core)
    twin = pltpu.make_async_remote_copy(
        src_ref=src_hbm,
        dst_ref=twin_ref,
        send_sem=twin_sem.at[0],
        recv_sem=twin_sem.at[1],
        device_id=(me, other),
        device_id_type=mesh_type,
    )
    gives = (core == 0) & (near_from == 1)
    takes = (core == 1) & (near_from == 1)
    before = sum((key(upper * mid + i) < key(me)).astype(jnp.int32) for i in range(mid))

    def announce(i):
        near = upper * mid + i

        @pl.when(key(near) < key(me))
        def _():
            pl.semaphore_signal(near_sem, inc=1, device_id=(near, core), device_id_type=mesh_type)

        @pl.when(upper == 1)
        def _():
            pl.semaphore_signal(
                flag_sem.at[me % mid], inc=1, device_id=(i, core), device_id_type=mesh_type
            )

    @pl.when(upper == 0)
    def _():
        pl.semaphore_wait(barrier, 1 + before)
        steps(mid, announce)
        pl.when(gives)(twin.start)
        swap.start()

    for load in inputs[:3]:
        load.wait()
    wide_tile[:, : tile_ref.shape[1]] = jnp.broadcast_to(
        tile_ref[...], (link_count, tile_ref.shape[1])
    )
    wide_cross[:, : cross_ref.shape[1]] = cross_ref[...]
    wide_row[:, : row_ref.shape[1]] = jnp.broadcast_to(
        row_ref[...], (link_count, row_ref.shape[1])
    )
    owners = -(-domains // LANES) * LANES
    around = lax.broadcasted_iota(jnp.int32, (1, owners), 1)
    lane = lax.broadcasted_iota(jnp.int32, (link_count, owners), 1)
    named = lookup(wide_row[...], wide_cross[...])
    rows = []
    for t in range(tiles):
        slot = jnp.minimum(lane * tiles + t, tile_ref.shape[1] - 1)
        rows.append(lookup(named, lookup(wide_tile[...], slot)))

    base = me * blocks
    locals_ = [
        jnp.where((row >= base) & (row < base + blocks), row - base, BIG) for row in rows
    ]
    last = jnp.full((1, owners), -1, jnp.int32)
    for j in range(per_owner):
        left = [jnp.where(at > last, at, BIG) for at in locals_]
        last = jnp.min(functools.reduce(jnp.minimum, left), axis=0, keepdims=True)
        index = jnp.minimum(last, blocks - 1)
        for d in range(domains):
            send_to[d * per_owner + j] = index[0, d]

    def fill(d):
        for j in range(per_owner):
            pack[pl.ds(d * planes + j * comps, comps)] = src_ref[send_to[d * per_owner + j]]

    inputs[3].wait()
    steps(domains, fill)
    for j in range(per_owner):
        buf[pl.ds(me * planes + j * comps, comps)] = src_ref[send_to[me * per_owner + j]]

    def exchange(to, box, start=0, number=full):
        return pltpu.make_async_remote_copy(
            src_ref=pack.at[pl.ds(to * planes + start, number)],
            dst_ref=buf.at[pl.ds(me * planes + start, number)],
            send_sem=send_sem,
            recv_sem=recv_sem.at[box],
            device_id=(to, core),
            device_id_type=mesh_type,
        )

    def across(to, **part):
        exchange(to, mailbox((me ^ to) % quarter), **part).start()

    def ready(to):
        wait_if(upper == 0, flag_sem.at[to % mid], 1)

    def first_of(i):
        to = me ^ (domains - 1 - i) ^ even ^ (lower * (quarter - 1))
        return jnp.where(plane == 2, i, to)

    def first(i):
        to = first_of(i)
        ready(to)
        across(to)

    def second(i, number=full):
        to = me ^ (mid + quarter - 1 - i) ^ even
        ready(to)
        across(to, number=number)

    def beside(known):
        def send(i):
            r = mid - 1 - i
            to = me ^ r

            @pl.when((key(to) < key(me)) == known)
            def _():
                exchange(to, r // quarter).start()

        if domains <= 16:
            steps(mid - 1, send)
        else:
            steps(quarter, send)
            steps(quarter - 1, lambda i: send(i + quarter))

    @pl.when(upper == 1)
    def _():
        pl.semaphore_wait(barrier, mid + 1 + before)
        steps(mid, announce)
        steps(quarter, first)

        @pl.when(jnp.logical_not(takes))
        def _():
            steps(quarter, second)

        pl.when(gives)(twin.start)
        swap.start()

    beside(True)
    wait_if(before < mid - 1, near_sem, mid - 1 - before)
    beside(False)

    @pl.when(upper == 0)
    def _():
        steps(quarter, first)

        @pl.when(jnp.logical_not(takes))
        def _():
            steps(quarter, second)

    def rim_of(i):
        to, lines = lower * mid + i, []
        for j in range(per_owner):
            block = twin_ref[send_to[to * per_owner + j]].astype(jnp.float32)
            lines.append(block[:, half - 1])
        if half > full:
            lines.append(jnp.zeros((half - full, cells), jnp.float32))
        pack[to * planes + full] = jnp.concatenate(lines, axis=0).astype(jnp.bfloat16)

    @pl.when(takes)
    def _():
        twin.wait_recv()
        steps(mid, rim_of)
        steps(quarter, lambda i: across(first_of(i), start=full, number=1))
        steps(quarter, lambda i: second(i, planes))

    link = lax.broadcasted_iota(jnp.int32, (link_count, owners), 0)
    mine = []
    for t in range(tiles):
        column = jnp.sum(jnp.where(lane == me, rows[t], 0), axis=1, keepdims=True)
        at = column - around * blocks
        mine.append(jnp.where((at >= 0) & (at < blocks), at, BIG))
    last = jnp.full((1, owners), -1, jnp.int32)
    for j in range(per_owner):
        least = [jnp.where(at > last, at, BIG) for at in mine]
        last = jnp.min(functools.reduce(jnp.minimum, least), axis=0, keepdims=True)
        one = jnp.full((link_count, owners), BIG, jnp.int32)
        two = jnp.full((link_count, owners), -1, jnp.int32)
        for t in range(tiles):
            hit = (mine[t] == last) & (last < BIG)
            one = jnp.minimum(one, jnp.where(hit, link + t * link_count, BIG))
            two = jnp.maximum(two, jnp.where(hit, link + t * link_count, -1))
        one = jnp.min(one, axis=0, keepdims=True)
        two = jnp.max(two, axis=0, keepdims=True)
        for i in range(domains):
            link_one[i * per_owner + j] = one[0, i]
            link_two[i * per_owner + j] = two[0, i]

    acc[...] = jnp.zeros_like(acc)

    def product(sources, rimmed=False):
        totals = [acc[t] for t in range(tiles)]
        outer = [[0.0] * tiles for _ in range(per_owner)]
        for frm in sources:
            for j in range(per_owner):
                here = buf[pl.ds(frm * planes + j * comps, comps)].astype(jnp.float32)
                lhs = here.reshape(count, cells)
                if rimmed:
                    rim = jnp.where(core == 1, buf[frm * planes + full].astype(jnp.float32), 0.0)
                    lhs = jnp.concatenate([lhs, rim], axis=0)
                lhs = lhs.astype(jnp.bfloat16)
                one = link_one[frm * per_owner + j]
                two = link_two[frm * per_owner + j]
                at_one, at_two = jnp.minimum(one, links - 1), jnp.maximum(two, 0)
                quad = jnp.concatenate(
                    [w_ref[0, at_one], w_ref[1, at_one], w_ref[0, at_two], w_ref[1, at_two]],
                    axis=1,
                )
                both = jnp.dot(lhs, quad, preferred_element_type=jnp.float32)
                for t in range(tiles):
                    begin, end = t * link_count, (t + 1) * link_count
                    part = jnp.where(
                        (one >= begin) & (one < end), both[:, : 2 * width], 0.0
                    ) + jnp.where((two >= begin) & (two < end), both[:, 2 * width :], 0.0)
                    totals[t] += part[:count]
                    if rimmed:
                        outer[j][t] += part[count:]
        for t in range(tiles):
            acc[t] = totals[t]
            if rimmed:
                parts = [outer[j][t][j * comps : (j + 1) * comps] for j in range(per_owner)]
                rim_acc[t] += sum(parts)

    def arrive(box, number):
        rows_in = buf.at[pl.ds(0, number)]
        pltpu.make_async_remote_copy(
            src_ref=rows_in,
            dst_ref=rows_in,
            send_sem=send_sem,
            recv_sem=recv_sem.at[box],
            device_id=(me, other),
            device_id_type=mesh_type,
        ).wait_recv()

    def beyond_mid(i, apart):
        return me ^ (mid + i) ^ (quarter * apart)

    load_w.wait()
    swap_to(other).wait_recv()

    far, near = 1 - near_from, near_from
    outmost = jnp.where(plane == 0, 1, 0)

    def own_half(i):
        return me ^ (quarter + i)

    def far_half(i):
        return beyond_mid(i, far)

    def near_half(i):
        return beyond_mid(i, near)

    rim_acc[...] = jnp.zeros_like(rim_acc)
    halo = pltpu.make_async_remote_copy(
        src_ref=edge,
        dst_ref=beyond,
        send_sem=edge_sem.at[0],
        recv_sem=edge_sem.at[1],
        device_id=(me, other),
        device_id_type=mesh_type,
    )

    def early_edge():
        now = acc[...].reshape(tiles, comps, half, 2 * width)
        edge[...] = now[:, :, half - 1]
        halo.start()

    if domains <= 16:
        product([me])
        arrive(0, (quarter - 1) * full)
        product([me ^ r for r in range(1, quarter)])
        arrive(1 + outmost, quarter * full)
        product([jnp.where(plane == 0, far_half(i), own_half(i)) for i in range(quarter)])
        arrive(2 - outmost, quarter * full)
        product([jnp.where(plane == 0, own_half(i), far_half(i)) for i in range(quarter)])
        pl.when(core == 0)(early_edge)
    else:
        arrive(0, (quarter - 1) * full)
        arrive(1, quarter * full)
        arrive(2, quarter * full)
        steps(mid, lambda r: product([me ^ r]))
        steps(quarter, lambda i: product([far_half(i)]))
        pl.when(core == 0)(early_edge)

    @pl.when(core == 0)
    def _():
        steps(quarter, lambda i: arrive(3 + i, full))

    @pl.when(core == 1)
    def _():
        steps(quarter, lambda i: arrive(3 + i, planes))

    if domains <= 16:
        product([near_half(i) for i in range(quarter)], rimmed=True)
    else:
        steps(quarter, lambda i: product([near_half(i)], rimmed=True))

    total = acc[...].reshape(tiles, comps, half, 2 * width)

    @pl.when(core == 1)
    def _():
        edge[...] = total[:, :, 0]
        halo.start()

    out_ref[0] = total.astype(jnp.bfloat16)

    def drain(number):
        sent = pack.at[pl.ds(0, number)]
        pltpu.make_async_remote_copy(
            src_ref=sent,
            dst_ref=sent,
            send_sem=send_sem,
            recv_sem=recv_sem.at[0],
            device_id=(me, other),
            device_id_type=mesh_type,
        ).wait_send()

    @pl.when(takes)
    def _():
        drain((domains - 1) * full + mid)

    @pl.when(jnp.logical_not(takes))
    def _():
        drain((domains - 1) * full)

    swap.wait_send()
    pl.when(gives)(twin.wait_send)
    halo.wait_recv()
    sample = lax.broadcasted_iota(jnp.int32, (half, 2 * width), 0)
    for t in range(tiles):
        past = beyond[t] + rim_acc[t]
        for p in range(comps):
            now = total[t, p]
            outer = jnp.broadcast_to(past[p : p + 1], now.shape)
            later = pltpu.roll(now, half - 1, 0)
            prior = pltpu.roll(now, 1, 0)
            later = jnp.where((sample == half - 1) & (core == 0), outer, later)
            prior = jnp.where((sample == 0) & (core == 1), outer, prior)
            rate = jnp.where(
                (sample == 0) & (core == 0),
                later - now,
                jnp.where(
                    (sample == half - 1) & (core == 1), now - prior, (later - prior) * 0.5
                ),
            )
            out_ref[1, t, p] = rate.astype(jnp.bfloat16)
    halo.wait_send()


def deliver(both_ref, source_ref, rate_ref, sem):
    copies = [
        pltpu.make_async_copy(both_ref.at[i], out, sem.at[i])
        for i, out in enumerate((source_ref, rate_ref))
    ]
    for copy in copies:
        copy.start()
    for copy in copies:
        copy.wait()


def shards(sources, weights, intersect, block_row, slot_tile):
    domains = lax.axis_size("dom")
    tiles, link_count, cells, width = weights.shape
    blocks, comps, half, _ = sources.shape
    links = tiles * link_count
    pool = links // 2
    per_owner = (pool + domains - 1) // domains
    vmem, smem = pltpu.VMEM, pltpu.SMEM
    shape = (tiles, comps, half, 2 * width)
    out = jax.ShapeDtypeStruct(shape, jnp.bfloat16)
    block = (half, cells)
    planes = per_owner * comps + 1
    dma, regular = pltpu.SemaphoreType.DMA, pltpu.SemaphoreType.REGULAR
    in_vmem = pl.BlockSpec(memory_space=vmem)
    anywhere = pl.BlockSpec(memory_space=pl.ANY)

    def wide(n):
        return vmem((link_count, -(-n // LANES) * LANES), jnp.int32)

    both = pl.pallas_call(
        functools.partial(kernel, domains, per_owner),
        out_shape=vmem((2,) + shape, jnp.bfloat16),
        in_specs=[anywhere] * 5,
        out_specs=in_vmem,
        scratch_shapes=[
            vmem((1, slot_tile.shape[0]), jnp.int32),
            vmem((1, block_row.shape[0]), jnp.int32),
            vmem((link_count, intersect.shape[0]), jnp.int32),
            vmem(sources.shape, jnp.bfloat16),
            wide(slot_tile.shape[0]),
            wide(block_row.shape[0]),
            wide(intersect.shape[0]),
            smem((domains * per_owner,), jnp.int32),
            smem((domains * per_owner,), jnp.int32),
            smem((domains * per_owner,), jnp.int32),
            vmem((2, links, cells, width), jnp.bfloat16),
            vmem((domains * planes,) + block, jnp.bfloat16),
            vmem((domains * planes,) + block, jnp.bfloat16),
            vmem((tiles, comps * half, 2 * width), jnp.float32),
            vmem((tiles, comps, 2 * width), jnp.float32),
            vmem((tiles, comps, 2 * width), jnp.float32),
            vmem(sources.shape, jnp.bfloat16),
            vmem((tiles, comps, 2 * width), jnp.float32),
            dma((4,)),
            dma,
            dma,
            dma((3 + domains // 4,)),
            dma,
            dma,
            dma((2,)),
            regular((domains // 2,)),
            regular,
            dma((2,)),
        ],
        compiler_params=pltpu.CompilerParams(collective_id=0, has_side_effects=True),
        cost_estimate=pl.CostEstimate(
            flops=4 * comps * half * weights.size,
            bytes_accessed=2 * weights.size,
            transcendentals=0,
        ),
    )(
        slot_tile.reshape(1, -1),
        block_row.reshape(1, -1),
        intersect.T,
        sources,
        weights.reshape(links, cells, width),
    )
    return pl.pallas_call(
        deliver,
        out_shape=(out, out),
        in_specs=[in_vmem],
        out_specs=(anywhere, anywhere),
        scratch_shapes=[dma((2,))],
    )(pltpu.with_memory_space_constraint(both, vmem))


def solution(mesh):
    return jax.shard_map(
        shards,
        mesh=mesh,
        in_specs=(P("dom", None, "tm", None), P("dom", None, None, "tm"), P(), P(), P()),
        out_specs=(P("dom", None, "tm", None), P("dom", None, "tm", None)),
        check_vma=False,
    )
```

```python
import functools

import jax
import jax.numpy as jnp
from jax import lax
from jax.experimental import pallas as pl
from jax.experimental.pallas import tpu as pltpu
from jax.sharding import PartitionSpec as P


BIG = 1 << 30
LANES = 128


def lookup(table, index):
    within, group = index & (LANES - 1), index >> 7
    outs = []
    for at in range(0, index.shape[1], LANES):
        value = jnp.zeros((index.shape[0], LANES), jnp.int32)
        for g in range(table.shape[1] // LANES):
            got = jnp.take_along_axis(
                table[:, g * LANES : (g + 1) * LANES],
                within[:, at : at + LANES],
                axis=1,
                mode="promise_in_bounds",
            )
            value = jnp.where(group[:, at : at + LANES] == g, got, value)
        outs.append(value)
    return outs[0] if len(outs) == 1 else jnp.concatenate(outs, axis=1)


def steps(count, body):
    if count <= 16:
        for i in range(count):
            body(i)
    else:
        def step(i, carry):
            body(i)
            return carry
        lax.fori_loop(0, count, step, 0)


def kernel(
    domains, per_owner,
    tile_hbm, row_hbm, cross_hbm, src_hbm, w_hbm, out_ref,
    tile_ref, row_ref, cross_ref, src_ref,
    wide_tile, wide_row, wide_cross, send_to, link_one, link_two,
    w_ref, pack, buf, acc, edge, beyond, twin_ref, rim_acc,
    in_sem, w_sem, send_sem, recv_sem, wsend_sem, wrecv_sem, edge_sem, flag_sem, near_sem,
    twin_sem,
):
    me = lax.axis_index("dom")
    core = lax.axis_index("tm")
    other = 1 - core
    links, width = w_ref.shape[1], w_ref.shape[3]
    blocks, comps, half, cells = src_ref.shape
    tiles = acc.shape[0]
    link_count = links // tiles
    count = comps * half
    full = per_owner * comps
    planes = full + 1
    mesh_type = pl.DeviceIdType.MESH
    mid, quarter = domains // 2, domains // 4
    upper = me // mid
    lower = 1 - upper
    plane = me // quarter
    inner = (plane + 1) // 2 % 2 * quarter
    even = (1 - plane % 2) * quarter

    def key(d):
        hops = d % 2 + d // 2 % 2 + d // quarter
        return (4 * hops - ((d // quarter - 1) % 4 == 1)) * domains + d

    def wait_if(condition, sem, value):
        @pl.when(condition)
        def _():
            pl.semaphore_wait(sem, value)

    near_from = inner // quarter

    def mailbox(offset):
        return 2 + near_from * (1 + offset)

    inputs = [
        pltpu.make_async_copy(source, target, in_sem.at[i])
        for i, (source, target) in enumerate(
            (
                (tile_hbm, tile_ref),
                (cross_hbm, cross_ref),
                (row_hbm, row_ref),
                (src_hbm, src_ref),
            )
        )
    ]
    for load in inputs:
        load.start()

    barrier = pltpu.get_barrier_semaphore()
    pl.semaphore_signal(barrier, inc=1, device_id=(me, other), device_id_type=mesh_type)

    def greet(i):
        to = domains - 1 - i

        @pl.when(key(to) > key(me))
        def _():
            pl.semaphore_signal(barrier, inc=1, device_id=(to, core), device_id_type=mesh_type)

    steps(domains, greet)

    load_w = pltpu.make_async_copy(w_hbm, w_ref.at[core], w_sem)
    load_w.start()

    wide_tile[...] = jnp.zeros_like(wide_tile)
    wide_cross[...] = jnp.zeros_like(wide_cross)
    wide_row[...] = jnp.zeros_like(wide_row)

    def swap_to(part):
        return pltpu.make_async_remote_copy(
            src_ref=w_hbm,
            dst_ref=w_ref.at[part],
            send_sem=wsend_sem,
            recv_sem=wrecv_sem,
            device_id=(me, other),
            device_id_type=mesh_type,
        )

    swap = swap_to(core)
    twin = pltpu.make_async_remote_copy(
        src_ref=src_hbm,
        dst_ref=twin_ref,
        send_sem=twin_sem.at[0],
        recv_sem=twin_sem.at[1],
        device_id=(me, other),
        device_id_type=mesh_type,
    )
    gives = (core == 0) & (near_from == 1)
    takes = (core == 1) & (near_from == 1)
    def below(start, number):
        return sum((key(start + i) < key(me)).astype(jnp.int32) for i in range(number))

    before, near_before = below(0, domains), below(upper * mid, mid)

    def announce(i):
        known = key(i) < key(me)

        @pl.when(known & (i // mid == upper))
        def _():
            pl.semaphore_signal(near_sem, inc=1, device_id=(i, core), device_id_type=mesh_type)

        @pl.when(known & (i // mid != upper))
        def _():
            pl.semaphore_signal(
                flag_sem.at[me % mid], inc=1, device_id=(i, core), device_id_type=mesh_type
            )

    for load in inputs[:3]:
        load.wait()
    wide_tile[:, : tile_ref.shape[1]] = jnp.broadcast_to(
        tile_ref[...], (link_count, tile_ref.shape[1])
    )
    wide_cross[:, : cross_ref.shape[1]] = cross_ref[...]
    wide_row[:, : row_ref.shape[1]] = jnp.broadcast_to(
        row_ref[...], (link_count, row_ref.shape[1])
    )
    owners = -(-domains // LANES) * LANES
    around = lax.broadcasted_iota(jnp.int32, (1, owners), 1)
    lane = lax.broadcasted_iota(jnp.int32, (link_count, owners), 1)
    named = lookup(wide_row[...], wide_cross[...])
    rows = []
    for t in range(tiles):
        slot = jnp.minimum(lane * tiles + t, tile_ref.shape[1] - 1)
        rows.append(lookup(named, lookup(wide_tile[...], slot)))

    base = me * blocks
    locals_ = [
        jnp.where((row >= base) & (row < base + blocks), row - base, BIG) for row in rows
    ]
    last = jnp.full((1, owners), -1, jnp.int32)
    for j in range(per_owner):
        left = [jnp.where(at > last, at, BIG) for at in locals_]
        last = jnp.min(functools.reduce(jnp.minimum, left), axis=0, keepdims=True)
        index = jnp.minimum(last, blocks - 1)
        for d in range(domains):
            send_to[d * per_owner + j] = index[0, d]

    def fill(d):
        for j in range(per_owner):
            pack[pl.ds(d * planes + j * comps, comps)] = src_ref[send_to[d * per_owner + j]]

    inputs[3].wait()
    steps(domains, fill)
    for j in range(per_owner):
        buf[pl.ds(me * planes + j * comps, comps)] = src_ref[send_to[me * per_owner + j]]

    def exchange(to, box, start=0, number=full):
        return pltpu.make_async_remote_copy(
            src_ref=pack.at[pl.ds(to * planes + start, number)],
            dst_ref=buf.at[pl.ds(me * planes + start, number)],
            send_sem=send_sem,
            recv_sem=recv_sem.at[box],
            device_id=(to, core),
            device_id_type=mesh_type,
        )

    def across(to, **part):
        exchange(to, mailbox((me ^ to) % quarter), **part).start()

    def ready(to):
        wait_if(key(to) > key(me), flag_sem.at[to % mid], 1)

    def first_of(i):
        to = me ^ (domains - 1 - i) ^ even
        return jnp.where(plane == 3, to, lower * mid + i)

    def first(i):
        to = first_of(i)
        ready(to)
        across(to)

    def second(i, number=full):
        to = me ^ (mid + quarter - 1 - i) ^ even
        ready(to)
        across(to, number=number)

    def beside(known):
        def send(i):
            r = mid - 1 - i
            to = me ^ r

            @pl.when((key(to) < key(me)) == known)
            def _():
                exchange(to, r // quarter).start()

        if domains <= 16:
            steps(mid - 1, send)
        else:
            steps(quarter, send)
            steps(quarter - 1, lambda i: send(i + quarter))

    pl.semaphore_wait(barrier, 1 + before)
    steps(domains, announce)
    pl.when(gives)(twin.start)
    swap.start()
    pl.when(upper == 0)(lambda: beside(True))
    steps(quarter, first)

    @pl.when(upper == 1)
    def _():
        @pl.when(jnp.logical_not(takes))
        def _():
            steps(quarter, second)

        beside(True)

    wait_if(near_before < mid - 1, near_sem, mid - 1 - near_before)
    beside(False)

    @pl.when((upper == 0) & jnp.logical_not(takes))
    def _():
        steps(quarter, second)

    def rim_of(i):
        to, lines = lower * mid + i, []
        for j in range(per_owner):
            block = twin_ref[send_to[to * per_owner + j]].astype(jnp.float32)
            lines.append(block[:, half - 1])
        if half > full:
            lines.append(jnp.zeros((half - full, cells), jnp.float32))
        pack[to * planes + full] = jnp.concatenate(lines, axis=0).astype(jnp.bfloat16)

    @pl.when(takes)
    def _():
        twin.wait_recv()
        steps(mid, rim_of)
        steps(quarter, lambda i: across(first_of(i), start=full, number=1))
        steps(quarter, lambda i: second(i, planes))

    link = lax.broadcasted_iota(jnp.int32, (link_count, owners), 0)
    mine = []
    for t in range(tiles):
        column = jnp.sum(jnp.where(lane == me, rows[t], 0), axis=1, keepdims=True)
        at = column - around * blocks
        mine.append(jnp.where((at >= 0) & (at < blocks), at, BIG))
    last = jnp.full((1, owners), -1, jnp.int32)
    for j in range(per_owner):
        least = [jnp.where(at > last, at, BIG) for at in mine]
        last = jnp.min(functools.reduce(jnp.minimum, least), axis=0, keepdims=True)
        one = jnp.full((link_count, owners), BIG, jnp.int32)
        two = jnp.full((link_count, owners), -1, jnp.int32)
        for t in range(tiles):
            hit = (mine[t] == last) & (last < BIG)
            one = jnp.minimum(one, jnp.where(hit, link + t * link_count, BIG))
            two = jnp.maximum(two, jnp.where(hit, link + t * link_count, -1))
        one = jnp.min(one, axis=0, keepdims=True)
        two = jnp.max(two, axis=0, keepdims=True)
        for i in range(domains):
            link_one[i * per_owner + j] = one[0, i]
            link_two[i * per_owner + j] = two[0, i]

    acc[...] = jnp.zeros_like(acc)

    def product(sources, rimmed=False):
        totals = [acc[t] for t in range(tiles)]
        outer = [[0.0] * tiles for _ in range(per_owner)]
        for frm in sources:
            for j in range(per_owner):
                here = buf[pl.ds(frm * planes + j * comps, comps)].astype(jnp.float32)
                lhs = here.reshape(count, cells)
                if rimmed:
                    rim = jnp.where(core == 1, buf[frm * planes + full].astype(jnp.float32), 0.0)
                    lhs = jnp.concatenate([lhs, rim], axis=0)
                lhs = lhs.astype(jnp.bfloat16)
                one = link_one[frm * per_owner + j]
                two = link_two[frm * per_owner + j]
                at_one, at_two = jnp.minimum(one, links - 1), jnp.maximum(two, 0)
                quad = jnp.concatenate(
                    [w_ref[0, at_one], w_ref[1, at_one], w_ref[0, at_two], w_ref[1, at_two]],
                    axis=1,
                )
                both = jnp.dot(lhs, quad, preferred_element_type=jnp.float32)
                for t in range(tiles):
                    begin, end = t * link_count, (t + 1) * link_count
                    part = jnp.where(
                        (one >= begin) & (one < end), both[:, : 2 * width], 0.0
                    ) + jnp.where((two >= begin) & (two < end), both[:, 2 * width :], 0.0)
                    totals[t] += part[:count]
                    if rimmed:
                        outer[j][t] += part[count:]
        for t in range(tiles):
            acc[t] = totals[t]
            if rimmed:
                parts = [outer[j][t][j * comps : (j + 1) * comps] for j in range(per_owner)]
                rim_acc[t] += sum(parts)

    def arrive(box, number):
        rows_in = buf.at[pl.ds(0, number)]
        pltpu.make_async_remote_copy(
            src_ref=rows_in,
            dst_ref=rows_in,
            send_sem=send_sem,
            recv_sem=recv_sem.at[box],
            device_id=(me, other),
            device_id_type=mesh_type,
        ).wait_recv()

    def beyond_mid(i, apart):
        return me ^ (mid + i) ^ (quarter * apart)

    load_w.wait()
    swap_to(other).wait_recv()

    far, near = 1 - near_from, near_from
    outmost = jnp.where(plane == 0, 1, 0)

    def own_half(i):
        return me ^ (quarter + i)

    def far_half(i):
        return beyond_mid(i, far)

    def near_half(i):
        return beyond_mid(i, near)

    rim_acc[...] = jnp.zeros_like(rim_acc)
    halo = pltpu.make_async_remote_copy(
        src_ref=edge,
        dst_ref=beyond,
        send_sem=edge_sem.at[0],
        recv_sem=edge_sem.at[1],
        device_id=(me, other),
        device_id_type=mesh_type,
    )

    def early_edge():
        now = acc[...].reshape(tiles, comps, half, 2 * width)
        edge[...] = now[:, :, half - 1]
        halo.start()

    if domains <= 16:
        product([me])
        arrive(0, (quarter - 1) * full)
        product([me ^ r for r in range(1, quarter)])
        arrive(1 + outmost, quarter * full)
        product([jnp.where(plane == 0, far_half(i), own_half(i)) for i in range(quarter)])
        arrive(2 - outmost, quarter * full)
        product([jnp.where(plane == 0, own_half(i), far_half(i)) for i in range(quarter)])
        pl.when(core == 0)(early_edge)
    else:
        arrive(0, (quarter - 1) * full)
        arrive(1, quarter * full)
        arrive(2, quarter * full)
        steps(mid, lambda r: product([me ^ r]))
        steps(quarter, lambda i: product([far_half(i)]))
        pl.when(core == 0)(early_edge)

    @pl.when(core == 0)
    def _():
        steps(quarter, lambda i: arrive(3 + i, full))

    @pl.when(core == 1)
    def _():
        steps(quarter, lambda i: arrive(3 + i, planes))

    if domains <= 16:
        product([near_half(i) for i in range(quarter)], rimmed=True)
    else:
        steps(quarter, lambda i: product([near_half(i)], rimmed=True))

    total = acc[...].reshape(tiles, comps, half, 2 * width)

    @pl.when(core == 1)
    def _():
        edge[...] = total[:, :, 0]
        halo.start()

    out_ref[0] = total.astype(jnp.bfloat16)

    def drain(number):
        sent = pack.at[pl.ds(0, number)]
        pltpu.make_async_remote_copy(
            src_ref=sent,
            dst_ref=sent,
            send_sem=send_sem,
            recv_sem=recv_sem.at[0],
            device_id=(me, other),
            device_id_type=mesh_type,
        ).wait_send()

    @pl.when(takes)
    def _():
        drain((domains - 1) * full + mid)

    @pl.when(jnp.logical_not(takes))
    def _():
        drain((domains - 1) * full)

    swap.wait_send()
    pl.when(gives)(twin.wait_send)
    halo.wait_recv()
    sample = lax.broadcasted_iota(jnp.int32, (half, 2 * width), 0)
    for t in range(tiles):
        past = beyond[t] + rim_acc[t]
        for p in range(comps):
            now = total[t, p]
            outer = jnp.broadcast_to(past[p : p + 1], now.shape)
            later = pltpu.roll(now, half - 1, 0)
            prior = pltpu.roll(now, 1, 0)
            later = jnp.where((sample == half - 1) & (core == 0), outer, later)
            prior = jnp.where((sample == 0) & (core == 1), outer, prior)
            rate = jnp.where(
                (sample == 0) & (core == 0),
                later - now,
                jnp.where(
                    (sample == half - 1) & (core == 1), now - prior, (later - prior) * 0.5
                ),
            )
            out_ref[1, t, p] = rate.astype(jnp.bfloat16)
    halo.wait_send()


def deliver(both_ref, source_ref, rate_ref, sem):
    copies = [
        pltpu.make_async_copy(both_ref.at[i], out, sem.at[i])
        for i, out in enumerate((source_ref, rate_ref))
    ]
    for copy in copies:
        copy.start()
    for copy in copies:
        copy.wait()


def shards(sources, weights, intersect, block_row, slot_tile):
    domains = lax.axis_size("dom")
    tiles, link_count, cells, width = weights.shape
    blocks, comps, half, _ = sources.shape
    links = tiles * link_count
    pool = links // 2
    per_owner = (pool + domains - 1) // domains
    vmem, smem = pltpu.VMEM, pltpu.SMEM
    shape = (tiles, comps, half, 2 * width)
    out = jax.ShapeDtypeStruct(shape, jnp.bfloat16)
    block = (half, cells)
    planes = per_owner * comps + 1
    dma, regular = pltpu.SemaphoreType.DMA, pltpu.SemaphoreType.REGULAR
    in_vmem = pl.BlockSpec(memory_space=vmem)
    anywhere = pl.BlockSpec(memory_space=pl.ANY)

    def wide(n):
        return vmem((link_count, -(-n // LANES) * LANES), jnp.int32)

    both = pl.pallas_call(
        functools.partial(kernel, domains, per_owner),
        out_shape=vmem((2,) + shape, jnp.bfloat16),
        in_specs=[anywhere] * 5,
        out_specs=in_vmem,
        scratch_shapes=[
            vmem((1, slot_tile.shape[0]), jnp.int32),
            vmem((1, block_row.shape[0]), jnp.int32),
            vmem((link_count, intersect.shape[0]), jnp.int32),
            vmem(sources.shape, jnp.bfloat16),
            wide(slot_tile.shape[0]),
            wide(block_row.shape[0]),
            wide(intersect.shape[0]),
            smem((domains * per_owner,), jnp.int32),
            smem((domains * per_owner,), jnp.int32),
            smem((domains * per_owner,), jnp.int32),
            vmem((2, links, cells, width), jnp.bfloat16),
            vmem((domains * planes,) + block, jnp.bfloat16),
            vmem((domains * planes,) + block, jnp.bfloat16),
            vmem((tiles, comps * half, 2 * width), jnp.float32),
            vmem((tiles, comps, 2 * width), jnp.float32),
            vmem((tiles, comps, 2 * width), jnp.float32),
            vmem(sources.shape, jnp.bfloat16),
            vmem((tiles, comps, 2 * width), jnp.float32),
            dma((4,)),
            dma,
            dma,
            dma((3 + domains // 4,)),
            dma,
            dma,
            dma((2,)),
            regular((domains // 2,)),
            regular,
            dma((2,)),
        ],
        compiler_params=pltpu.CompilerParams(collective_id=0, has_side_effects=True),
        cost_estimate=pl.CostEstimate(
            flops=4 * comps * half * weights.size,
            bytes_accessed=2 * weights.size,
            transcendentals=0,
        ),
    )(
        slot_tile.reshape(1, -1),
        block_row.reshape(1, -1),
        intersect.T,
        sources,
        weights.reshape(links, cells, width),
    )
    return pl.pallas_call(
        deliver,
        out_shape=(out, out),
        in_specs=[in_vmem],
        out_specs=(anywhere, anywhere),
        scratch_shapes=[dma((2,))],
    )(pltpu.with_memory_space_constraint(both, vmem))


def solution(mesh):
    return jax.shard_map(
        shards,
        mesh=mesh,
        in_specs=(P("dom", None, "tm", None), P("dom", None, None, "tm"), P(), P(), P()),
        out_specs=(P("dom", None, "tm", None), P("dom", None, "tm", None)),
        check_vma=False,
    )
```

```python
import functools

import jax
import jax.numpy as jnp
from jax import lax
from jax.experimental import pallas as pl
from jax.experimental.pallas import tpu as pltpu
from jax.sharding import PartitionSpec as P


BIG = 1 << 30
LANES = 128


def lookup(table, index):
    within, group = index & (LANES - 1), index >> 7
    outs = []
    for at in range(0, index.shape[1], LANES):
        value = jnp.zeros((index.shape[0], LANES), jnp.int32)
        for g in range(table.shape[1] // LANES):
            got = jnp.take_along_axis(
                table[:, g * LANES : (g + 1) * LANES],
                within[:, at : at + LANES],
                axis=1,
                mode="promise_in_bounds",
            )
            value = jnp.where(group[:, at : at + LANES] == g, got, value)
        outs.append(value)
    return outs[0] if len(outs) == 1 else jnp.concatenate(outs, axis=1)


def steps(count, body):
    if count <= 16:
        for i in range(count):
            body(i)
    else:
        def step(i, carry):
            body(i)
            return carry
        lax.fori_loop(0, count, step, 0)


def kernel(
    domains, per_owner,
    tile_hbm, row_hbm, cross_hbm, src_hbm, w_hbm, out_ref,
    tile_ref, row_ref, cross_ref, src_ref,
    wide_tile, wide_row, wide_cross, send_to, link_one, link_two,
    w_ref, pack, buf, acc, edge, beyond, twin_ref, rim_acc,
    in_sem, w_sem, send_sem, recv_sem, wsend_sem, wrecv_sem, edge_sem, flag_sem, near_sem,
    twin_sem,
):
    me = lax.axis_index("dom")
    core = lax.axis_index("tm")
    other = 1 - core
    links, width = w_ref.shape[1], w_ref.shape[3]
    blocks, comps, half, cells = src_ref.shape
    tiles = acc.shape[0]
    link_count = links // tiles
    count = comps * half
    full = per_owner * comps
    planes = full + 1
    mesh_type = pl.DeviceIdType.MESH
    mid, quarter = domains // 2, domains // 4
    upper = me // mid
    lower = 1 - upper
    plane = me // quarter
    inner = (plane + 1) // 2 % 2 * quarter
    even = (1 - plane % 2) * quarter

    def key(d):
        hops = d % 2 + d // 2 % 2 + d // quarter
        shift = (0, 0, -1, 4)
        moved = sum(shift[p] * (d // quarter == p) for p in range(4))
        return (4 * hops + moved) * domains + d

    def wait_if(condition, sem, value):
        @pl.when(condition)
        def _():
            pl.semaphore_wait(sem, value)

    near_from = inner // quarter

    def mailbox(offset):
        return 2 + near_from * (1 + offset)

    inputs = [
        pltpu.make_async_copy(source, target, in_sem.at[i])
        for i, (source, target) in enumerate(
            (
                (tile_hbm, tile_ref),
                (cross_hbm, cross_ref),
                (row_hbm, row_ref),
                (src_hbm, src_ref),
            )
        )
    ]
    for load in inputs:
        load.start()

    barrier = pltpu.get_barrier_semaphore()
    pl.semaphore_signal(barrier, inc=1, device_id=(me, other), device_id_type=mesh_type)

    def greet(i):
        to = domains - 1 - i

        @pl.when(key(to) > key(me))
        def _():
            pl.semaphore_signal(barrier, inc=1, device_id=(to, core), device_id_type=mesh_type)

    steps(domains, greet)

    load_w = pltpu.make_async_copy(w_hbm, w_ref.at[core], w_sem)
    load_w.start()

    wide_tile[...] = jnp.zeros_like(wide_tile)
    wide_cross[...] = jnp.zeros_like(wide_cross)
    wide_row[...] = jnp.zeros_like(wide_row)

    def swap_to(part):
        return pltpu.make_async_remote_copy(
            src_ref=w_hbm,
            dst_ref=w_ref.at[part],
            send_sem=wsend_sem,
            recv_sem=wrecv_sem,
            device_id=(me, other),
            device_id_type=mesh_type,
        )

    swap = swap_to(core)
    twin = pltpu.make_async_remote_copy(
        src_ref=src_hbm,
        dst_ref=twin_ref,
        send_sem=twin_sem.at[0],
        recv_sem=twin_sem.at[1],
        device_id=(me, other),
        device_id_type=mesh_type,
    )
    gives = (core == 0) & (near_from == 1)
    takes = (core == 1) & (near_from == 1)
    def below(start, number):
        return sum((key(start + i) < key(me)).astype(jnp.int32) for i in range(number))

    before, near_before = below(0, domains), below(upper * mid, mid)

    def announce(i):
        known = key(i) < key(me)

        @pl.when(known & (i // mid == upper))
        def _():
            pl.semaphore_signal(near_sem, inc=1, device_id=(i, core), device_id_type=mesh_type)

        @pl.when(known & (i // mid != upper))
        def _():
            pl.semaphore_signal(
                flag_sem.at[me % mid], inc=1, device_id=(i, core), device_id_type=mesh_type
            )

    for load in inputs[:3]:
        load.wait()
    wide_tile[:, : tile_ref.shape[1]] = jnp.broadcast_to(
        tile_ref[...], (link_count, tile_ref.shape[1])
    )
    wide_cross[:, : cross_ref.shape[1]] = cross_ref[...]
    wide_row[:, : row_ref.shape[1]] = jnp.broadcast_to(
        row_ref[...], (link_count, row_ref.shape[1])
    )
    owners = -(-domains // LANES) * LANES
    around = lax.broadcasted_iota(jnp.int32, (1, owners), 1)
    lane = lax.broadcasted_iota(jnp.int32, (link_count, owners), 1)
    named = lookup(wide_row[...], wide_cross[...])
    rows = []
    for t in range(tiles):
        slot = jnp.minimum(lane * tiles + t, tile_ref.shape[1] - 1)
        rows.append(lookup(named, lookup(wide_tile[...], slot)))

    base = me * blocks
    locals_ = [
        jnp.where((row >= base) & (row < base + blocks), row - base, BIG) for row in rows
    ]
    last = jnp.full((1, owners), -1, jnp.int32)
    for j in range(per_owner):
        left = [jnp.where(at > last, at, BIG) for at in locals_]
        last = jnp.min(functools.reduce(jnp.minimum, left), axis=0, keepdims=True)
        index = jnp.minimum(last, blocks - 1)
        for d in range(domains):
            send_to[d * per_owner + j] = index[0, d]

    def fill(d):
        for j in range(per_owner):
            pack[pl.ds(d * planes + j * comps, comps)] = src_ref[send_to[d * per_owner + j]]

    inputs[3].wait()
    steps(domains, fill)
    for j in range(per_owner):
        buf[pl.ds(me * planes + j * comps, comps)] = src_ref[send_to[me * per_owner + j]]

    def exchange(to, box, start=0, number=full):
        return pltpu.make_async_remote_copy(
            src_ref=pack.at[pl.ds(to * planes + start, number)],
            dst_ref=buf.at[pl.ds(me * planes + start, number)],
            send_sem=send_sem,
            recv_sem=recv_sem.at[box],
            device_id=(to, core),
            device_id_type=mesh_type,
        )

    def across(to, **part):
        exchange(to, mailbox((me ^ to) % quarter), **part).start()

    def ready(to):
        wait_if(key(to) > key(me), flag_sem.at[to % mid], 1)

    def first_of(i):
        to = me ^ (domains - 1 - i) ^ even
        return jnp.where(plane == 3, to, lower * mid + i)

    def first(i, **part):
        to = first_of(i)
        ready(to)
        across(to, **part)

    def second(i, **part):
        to = me ^ (mid + quarter - 1 - i) ^ even
        ready(to)
        across(to, **part)

    def beside(known):
        def send(i):
            r = mid - 1 - i
            to = me ^ r

            @pl.when((key(to) < key(me)) == known)
            def _():
                exchange(to, r // quarter).start()

        if domains <= 16:
            steps(mid - 1, send)
        else:
            steps(quarter, send)
            steps(quarter - 1, lambda i: send(i + quarter))

    pl.semaphore_wait(barrier, 1 + before)
    steps(domains, announce)
    pl.when(gives)(twin.start)
    swap.start()
    def rim_of(i):
        to, lines = lower * mid + i, []
        for j in range(per_owner):
            block = twin_ref[send_to[to * per_owner + j]].astype(jnp.float32)
            lines.append(block[:, half - 1])
        if half > full:
            lines.append(jnp.zeros((half - full, cells), jnp.float32))
        pack[to * planes + full] = jnp.concatenate(lines, axis=0).astype(jnp.bfloat16)

    early = quarter - 1

    def fork(send, start, number):
        @pl.when(takes)
        def _():
            steps(number, lambda i: send(i + start, number=planes))

        @pl.when(jnp.logical_not(takes))
        def _():
            steps(number, lambda i: send(i + start))

    pl.when(upper == 0)(lambda: beside(True))
    steps(early, first)

    @pl.when(takes)
    def _():
        twin.wait_recv()
        steps(mid, rim_of)
        steps(early, lambda i: across(first_of(i), start=full, number=1))

    fork(first, early, quarter - early)

    @pl.when(upper == 1)
    def _():
        fork(second, 0, quarter)
        beside(True)

    wait_if(near_before < mid - 1, near_sem, mid - 1 - near_before)
    beside(False)
    pl.when(upper == 0)(lambda: fork(second, 0, quarter))

    link = lax.broadcasted_iota(jnp.int32, (link_count, owners), 0)
    mine = []
    for t in range(tiles):
        column = jnp.sum(jnp.where(lane == me, rows[t], 0), axis=1, keepdims=True)
        at = column - around * blocks
        mine.append(jnp.where((at >= 0) & (at < blocks), at, BIG))
    last = jnp.full((1, owners), -1, jnp.int32)
    for j in range(per_owner):
        least = [jnp.where(at > last, at, BIG) for at in mine]
        last = jnp.min(functools.reduce(jnp.minimum, least), axis=0, keepdims=True)
        one = jnp.full((link_count, owners), BIG, jnp.int32)
        two = jnp.full((link_count, owners), -1, jnp.int32)
        for t in range(tiles):
            hit = (mine[t] == last) & (last < BIG)
            one = jnp.minimum(one, jnp.where(hit, link + t * link_count, BIG))
            two = jnp.maximum(two, jnp.where(hit, link + t * link_count, -1))
        one = jnp.min(one, axis=0, keepdims=True)
        two = jnp.max(two, axis=0, keepdims=True)
        for i in range(domains):
            link_one[i * per_owner + j] = one[0, i]
            link_two[i * per_owner + j] = two[0, i]

    acc[...] = jnp.zeros_like(acc)

    def product(sources, rimmed=False):
        totals = [acc[t] for t in range(tiles)]
        outer = [[0.0] * tiles for _ in range(per_owner)]
        for frm in sources:
            for j in range(per_owner):
                here = buf[pl.ds(frm * planes + j * comps, comps)].astype(jnp.float32)
                lhs = here.reshape(count, cells)
                if rimmed:
                    rim = jnp.where(core == 1, buf[frm * planes + full].astype(jnp.float32), 0.0)
                    lhs = jnp.concatenate([lhs, rim], axis=0)
                lhs = lhs.astype(jnp.bfloat16)
                one = link_one[frm * per_owner + j]
                two = link_two[frm * per_owner + j]
                at_one, at_two = jnp.minimum(one, links - 1), jnp.maximum(two, 0)
                quad = jnp.concatenate(
                    [w_ref[0, at_one], w_ref[1, at_one], w_ref[0, at_two], w_ref[1, at_two]],
                    axis=1,
                )
                both = jnp.dot(lhs, quad, preferred_element_type=jnp.float32)
                for t in range(tiles):
                    begin, end = t * link_count, (t + 1) * link_count
                    part = jnp.where(
                        (one >= begin) & (one < end), both[:, : 2 * width], 0.0
                    ) + jnp.where((two >= begin) & (two < end), both[:, 2 * width :], 0.0)
                    totals[t] += part[:count]
                    if rimmed:
                        outer[j][t] += part[count:]
        for t in range(tiles):
            acc[t] = totals[t]
            if rimmed:
                parts = [outer[j][t][j * comps : (j + 1) * comps] for j in range(per_owner)]
                rim_acc[t] += sum(parts)

    def arrive(box, number):
        rows_in = buf.at[pl.ds(0, number)]
        pltpu.make_async_remote_copy(
            src_ref=rows_in,
            dst_ref=rows_in,
            send_sem=send_sem,
            recv_sem=recv_sem.at[box],
            device_id=(me, other),
            device_id_type=mesh_type,
        ).wait_recv()

    def beyond_mid(i, apart):
        return me ^ (mid + i) ^ (quarter * apart)

    load_w.wait()
    swap_to(other).wait_recv()

    far, near = 1 - near_from, near_from
    outmost = jnp.where(plane == 0, 1, 0)

    def own_half(i):
        return me ^ (quarter + i)

    def far_half(i):
        return beyond_mid(i, far)

    def near_half(i):
        return beyond_mid(i, near)

    rim_acc[...] = jnp.zeros_like(rim_acc)
    halo = pltpu.make_async_remote_copy(
        src_ref=edge,
        dst_ref=beyond,
        send_sem=edge_sem.at[0],
        recv_sem=edge_sem.at[1],
        device_id=(me, other),
        device_id_type=mesh_type,
    )

    def early_edge():
        now = acc[...].reshape(tiles, comps, half, 2 * width)
        edge[...] = now[:, :, half - 1]
        halo.start()

    if domains <= 16:
        product([me])
        arrive(0, (quarter - 1) * full)
        product([me ^ r for r in range(1, quarter)])
        arrive(1 + outmost, quarter * full)
        product([jnp.where(plane == 0, far_half(i), own_half(i)) for i in range(quarter)])
        arrive(2 - outmost, quarter * full)
        product([jnp.where(plane == 0, own_half(i), far_half(i)) for i in range(quarter)])
        pl.when(core == 0)(early_edge)
    else:
        arrive(0, (quarter - 1) * full)
        arrive(1, quarter * full)
        arrive(2, quarter * full)
        steps(mid, lambda r: product([me ^ r]))
        steps(quarter, lambda i: product([far_half(i)]))
        pl.when(core == 0)(early_edge)

    def arrive_near(offset):
        @pl.when(core == 0)
        def _():
            arrive(3 + offset, full)

        @pl.when(core == 1)
        def _():
            arrive(3 + offset, planes)

    def offset_of(i):
        by_column = lower * other
        return by_column * (i ^ (me % quarter)) + (1 - by_column) * (quarter - 1 - i)

    if domains <= 16:
        for i in range(0, quarter, 2):
            pair = [offset_of(i), offset_of(i + 1)]
            for offset in pair:
                arrive_near(offset)
            product([near_half(offset) for offset in pair], rimmed=True)
    else:
        steps(quarter, arrive_near)
        steps(quarter, lambda i: product([near_half(i)], rimmed=True))

    total = acc[...].reshape(tiles, comps, half, 2 * width)

    @pl.when(core == 1)
    def _():
        edge[...] = total[:, :, 0]
        halo.start()

    out_ref[0] = total.astype(jnp.bfloat16)

    def drain(number):
        sent = pack.at[pl.ds(0, number)]
        pltpu.make_async_remote_copy(
            src_ref=sent,
            dst_ref=sent,
            send_sem=send_sem,
            recv_sem=recv_sem.at[0],
            device_id=(me, other),
            device_id_type=mesh_type,
        ).wait_send()

    @pl.when(takes)
    def _():
        drain((domains - 1) * full + mid)

    @pl.when(jnp.logical_not(takes))
    def _():
        drain((domains - 1) * full)

    swap.wait_send()
    pl.when(gives)(twin.wait_send)
    halo.wait_recv()
    sample = lax.broadcasted_iota(jnp.int32, (half, 2 * width), 0)
    for t in range(tiles):
        past = beyond[t] + rim_acc[t]
        for p in range(comps):
            now = total[t, p]
            outer = jnp.broadcast_to(past[p : p + 1], now.shape)
            later = pltpu.roll(now, half - 1, 0)
            prior = pltpu.roll(now, 1, 0)
            later = jnp.where((sample == half - 1) & (core == 0), outer, later)
            prior = jnp.where((sample == 0) & (core == 1), outer, prior)
            rate = jnp.where(
                (sample == 0) & (core == 0),
                later - now,
                jnp.where(
                    (sample == half - 1) & (core == 1), now - prior, (later - prior) * 0.5
                ),
            )
            out_ref[1, t, p] = rate.astype(jnp.bfloat16)
    halo.wait_send()


def deliver(both_ref, source_ref, rate_ref, sem):
    copies = [
        pltpu.make_async_copy(both_ref.at[i], out, sem.at[i])
        for i, out in enumerate((source_ref, rate_ref))
    ]
    for copy in copies:
        copy.start()
    for copy in copies:
        copy.wait()


def shards(sources, weights, intersect, block_row, slot_tile):
    domains = lax.axis_size("dom")
    tiles, link_count, cells, width = weights.shape
    blocks, comps, half, _ = sources.shape
    links = tiles * link_count
    pool = links // 2
    per_owner = (pool + domains - 1) // domains
    vmem, smem = pltpu.VMEM, pltpu.SMEM
    shape = (tiles, comps, half, 2 * width)
    out = jax.ShapeDtypeStruct(shape, jnp.bfloat16)
    block = (half, cells)
    planes = per_owner * comps + 1
    dma, regular = pltpu.SemaphoreType.DMA, pltpu.SemaphoreType.REGULAR
    in_vmem = pl.BlockSpec(memory_space=vmem)
    anywhere = pl.BlockSpec(memory_space=pl.ANY)

    def wide(n):
        return vmem((link_count, -(-n // LANES) * LANES), jnp.int32)

    both = pl.pallas_call(
        functools.partial(kernel, domains, per_owner),
        out_shape=vmem((2,) + shape, jnp.bfloat16),
        in_specs=[anywhere] * 5,
        out_specs=in_vmem,
        scratch_shapes=[
            vmem((1, slot_tile.shape[0]), jnp.int32),
            vmem((1, block_row.shape[0]), jnp.int32),
            vmem((link_count, intersect.shape[0]), jnp.int32),
            vmem(sources.shape, jnp.bfloat16),
            wide(slot_tile.shape[0]),
            wide(block_row.shape[0]),
            wide(intersect.shape[0]),
            smem((domains * per_owner,), jnp.int32),
            smem((domains * per_owner,), jnp.int32),
            smem((domains * per_owner,), jnp.int32),
            vmem((2, links, cells, width), jnp.bfloat16),
            vmem((domains * planes,) + block, jnp.bfloat16),
            vmem((domains * planes,) + block, jnp.bfloat16),
            vmem((tiles, comps * half, 2 * width), jnp.float32),
            vmem((tiles, comps, 2 * width), jnp.float32),
            vmem((tiles, comps, 2 * width), jnp.float32),
            vmem(sources.shape, jnp.bfloat16),
            vmem((tiles, comps, 2 * width), jnp.float32),
            dma((4,)),
            dma,
            dma,
            dma((3 + domains // 4,)),
            dma,
            dma,
            dma((2,)),
            regular((domains // 2,)),
            regular,
            dma((2,)),
        ],
        compiler_params=pltpu.CompilerParams(collective_id=0, has_side_effects=True),
        cost_estimate=pl.CostEstimate(
            flops=4 * comps * half * weights.size,
            bytes_accessed=2 * weights.size,
            transcendentals=0,
        ),
    )(
        slot_tile.reshape(1, -1),
        block_row.reshape(1, -1),
        intersect.T,
        sources,
        weights.reshape(links, cells, width),
    )
    return pl.pallas_call(
        deliver,
        out_shape=(out, out),
        in_specs=[in_vmem],
        out_specs=(anywhere, anywhere),
        scratch_shapes=[dma((2,))],
    )(pltpu.with_memory_space_constraint(both, vmem))


def solution(mesh):
    return jax.shard_map(
        shards,
        mesh=mesh,
        in_specs=(P("dom", None, "tm", None), P("dom", None, None, "tm"), P(), P(), P()),
        out_specs=(P("dom", None, "tm", None), P("dom", None, "tm", None)),
        check_vma=False,
    )
```

```python
import functools

import jax
import jax.numpy as jnp
from jax import lax
from jax.experimental import pallas as pl
from jax.experimental.pallas import tpu as pltpu
from jax.sharding import PartitionSpec as P


BIG = 1 << 30
LANES = 128


def lookup(table, index):
    within, group = index & (LANES - 1), index >> 7
    outs = []
    for at in range(0, index.shape[1], LANES):
        value = jnp.zeros((index.shape[0], LANES), jnp.int32)
        for g in range(table.shape[1] // LANES):
            got = jnp.take_along_axis(
                table[:, g * LANES : (g + 1) * LANES],
                within[:, at : at + LANES],
                axis=1,
                mode="promise_in_bounds",
            )
            value = jnp.where(group[:, at : at + LANES] == g, got, value)
        outs.append(value)
    return outs[0] if len(outs) == 1 else jnp.concatenate(outs, axis=1)


def steps(count, body):
    if count <= 16:
        for i in range(count):
            body(i)
    else:
        def step(i, carry):
            body(i)
            return carry
        lax.fori_loop(0, count, step, 0)


def kernel(
    domains, per_owner,
    tile_hbm, row_hbm, cross_hbm, src_hbm, w_hbm, out_ref,
    tile_ref, row_ref, cross_ref, src_ref,
    wide_tile, wide_row, wide_cross, send_to, link_one, link_two,
    w_ref, pack, buf, acc, edge, beyond, twin_ref, rim_acc, rim_out, rim_in,
    in_sem, w_sem, send_sem, recv_sem, side_sem, wrecv_sem, edge_sem, flag_sem, near_sem,
    twin_sem, rim_sem,
):
    me = lax.axis_index("dom")
    core = lax.axis_index("tm")
    other = 1 - core
    links, width = w_ref.shape[1], w_ref.shape[3]
    blocks, comps, half, cells = src_ref.shape
    tiles = acc.shape[0]
    link_count = links // tiles
    count = comps * half
    full = per_owner * comps
    planes = full + 1
    mesh_type = pl.DeviceIdType.MESH
    mid, quarter = domains // 2, domains // 4
    upper = me // mid
    lower = 1 - upper
    plane = me // quarter
    inner = (plane + 1) // 2 % 2 * quarter
    even = (1 - plane % 2) * quarter

    def key(d):
        hops = d % 2 + d // 2 % 2 + d // quarter
        shift = (0, 0, -1, 4)
        moved = sum(shift[p] * (d // quarter == p) for p in range(4))
        return (4 * hops + moved) * domains + d

    def wait_if(condition, sem, value):
        @pl.when(condition)
        def _():
            pl.semaphore_wait(sem, value)

    near_from = inner // quarter

    def mailbox(offset):
        return 2 + near_from * (1 + offset)

    inputs = [
        pltpu.make_async_copy(source, target, in_sem.at[i // 3])
        for i, (source, target) in enumerate(
            (
                (tile_hbm, tile_ref),
                (cross_hbm, cross_ref),
                (row_hbm, row_ref),
                (src_hbm, src_ref),
            )
        )
    ]
    for load in inputs:
        load.start()

    barrier = pltpu.get_barrier_semaphore()
    pl.semaphore_signal(barrier, inc=1, device_id=(me, other), device_id_type=mesh_type)

    def greet(i):
        to = domains - 1 - i

        @pl.when(key(to) > key(me))
        def _():
            pl.semaphore_signal(barrier, inc=1, device_id=(to, core), device_id_type=mesh_type)

    steps(domains, greet)

    load_w = pltpu.make_async_copy(w_hbm, w_ref.at[core], w_sem)
    load_w.start()

    wide_tile[...] = jnp.zeros_like(wide_tile)
    wide_cross[...] = jnp.zeros_like(wide_cross)
    wide_row[...] = jnp.zeros_like(wide_row)

    def swap_to(part):
        return pltpu.make_async_remote_copy(
            src_ref=w_hbm,
            dst_ref=w_ref.at[part],
            send_sem=side_sem,
            recv_sem=wrecv_sem,
            device_id=(me, other),
            device_id_type=mesh_type,
        )

    swap = swap_to(core)
    twin = pltpu.make_async_remote_copy(
        src_ref=src_hbm,
        dst_ref=twin_ref,
        send_sem=side_sem,
        recv_sem=twin_sem,
        device_id=(me, other),
        device_id_type=mesh_type,
    )
    gives = (core == 0) & (near_from == 1)
    takes = (core == 1) & (near_from == 1)
    def below(start, number):
        return sum((key(start + i) < key(me)).astype(jnp.int32) for i in range(number))

    before, near_before = below(0, domains), below(upper * mid, mid)

    flag = me % quarter + plane % 2 * (quarter - me % quarter)

    def announce(i):
        known = key(i) < key(me)

        @pl.when(known & (i // mid == upper))
        def _():
            pl.semaphore_signal(near_sem, inc=1, device_id=(i, core), device_id_type=mesh_type)

        @pl.when(known & (i // mid != upper))
        def _():
            pl.semaphore_signal(
                flag_sem.at[flag], inc=1, device_id=(i, core), device_id_type=mesh_type
            )

    for load in inputs[:3]:
        load.wait()
    wide_tile[:, : tile_ref.shape[1]] = jnp.broadcast_to(
        tile_ref[...], (link_count, tile_ref.shape[1])
    )
    wide_cross[:, : cross_ref.shape[1]] = cross_ref[...]
    wide_row[:, : row_ref.shape[1]] = jnp.broadcast_to(
        row_ref[...], (link_count, row_ref.shape[1])
    )
    owners = -(-domains // LANES) * LANES
    around = lax.broadcasted_iota(jnp.int32, (1, owners), 1)
    lane = lax.broadcasted_iota(jnp.int32, (link_count, owners), 1)
    named = lookup(wide_row[...], wide_cross[...])
    rows = []
    for t in range(tiles):
        slot = jnp.minimum(lane * tiles + t, tile_ref.shape[1] - 1)
        rows.append(lookup(named, lookup(wide_tile[...], slot)))

    base = me * blocks
    locals_ = [
        jnp.where((row >= base) & (row < base + blocks), row - base, BIG) for row in rows
    ]
    last = jnp.full((1, owners), -1, jnp.int32)
    for j in range(per_owner):
        left = [jnp.where(at > last, at, BIG) for at in locals_]
        last = jnp.min(functools.reduce(jnp.minimum, left), axis=0, keepdims=True)
        index = jnp.minimum(last, blocks - 1)
        for d in range(domains):
            send_to[d * per_owner + j] = index[0, d]

    def fill(d):
        for j in range(per_owner):
            pack[pl.ds(d * planes + j * comps, comps)] = src_ref[send_to[d * per_owner + j]]

    inputs[3].wait()
    steps(domains, fill)
    for j in range(per_owner):
        buf[pl.ds(me * planes + j * comps, comps)] = src_ref[send_to[me * per_owner + j]]

    def exchange(to, box, start=0, number=full):
        return pltpu.make_async_remote_copy(
            src_ref=pack.at[pl.ds(to * planes + start, number)],
            dst_ref=buf.at[pl.ds(me * planes + start, number)],
            send_sem=send_sem,
            recv_sem=recv_sem.at[box],
            device_id=(to, core),
            device_id_type=mesh_type,
        )

    def across(to, **part):
        exchange(to, mailbox((me ^ to) % quarter), **part).start()

    def first_of(i):
        to = me ^ (domains - 1 - i) ^ even
        return jnp.where(plane == 3, to, lower * mid + i)

    def first(i, **part):
        to = first_of(i)
        wait_if(key(to) > key(me), flag_sem.at[to % quarter], 1)
        across(to, **part)

    def second(i, **part):
        across(me ^ (mid + quarter - 1 - i) ^ even, **part)

    def beside(known):
        def send(i):
            r = mid - 1 - i
            to = me ^ r

            @pl.when((key(to) < key(me)) == known)
            def _():
                exchange(to, r // quarter).start()

        if domains <= 16:
            steps(mid - 1, send)
        else:
            steps(quarter, send)
            steps(quarter - 1, lambda i: send(i + quarter))

    pl.semaphore_wait(barrier, 1 + before)
    steps(domains, announce)
    pl.when(gives)(twin.start)
    swap.start()
    def rim_of(i):
        to, lines = lower * mid + i, []
        for j in range(per_owner):
            block = twin_ref[send_to[to * per_owner + j]].astype(jnp.float32)
            lines.append(block[:, half - 1])
        if half > full:
            lines.append(jnp.zeros((half - full, cells), jnp.float32))
        pack[to * planes + full] = jnp.concatenate(lines, axis=0).astype(jnp.bfloat16)

    early = quarter - 1

    def fork(send, start, number):
        @pl.when(takes)
        def _():
            steps(number, lambda i: send(i + start, number=planes))

        @pl.when(jnp.logical_not(takes))
        def _():
            steps(number, lambda i: send(i + start))

    pl.when(upper == 0)(lambda: beside(True))
    steps(early, first)

    @pl.when(takes)
    def _():
        twin.wait_recv()
        steps(mid, rim_of)
        steps(early, lambda i: across(first_of(i), start=full, number=1))

    fork(first, early, quarter - early)

    later = lower * mid + quarter
    due = quarter - below(later, quarter)

    @pl.when(upper == 1)
    def _():
        wait_if(due > 0, flag_sem.at[quarter], due)
        fork(second, 0, quarter)
        beside(True)

    wait_if(near_before < mid - 1, near_sem, mid - 1 - near_before)
    beside(False)

    @pl.when(upper == 0)
    def _():
        pl.semaphore_wait(flag_sem.at[quarter], due)
        fork(second, 0, quarter)


    link = lax.broadcasted_iota(jnp.int32, (link_count, owners), 0)
    mine = []
    for t in range(tiles):
        column = jnp.sum(jnp.where(lane == me, rows[t], 0), axis=1, keepdims=True)
        at = column - around * blocks
        mine.append(jnp.where((at >= 0) & (at < blocks), at, BIG))
    last = jnp.full((1, owners), -1, jnp.int32)
    for j in range(per_owner):
        least = [jnp.where(at > last, at, BIG) for at in mine]
        last = jnp.min(functools.reduce(jnp.minimum, least), axis=0, keepdims=True)
        one = jnp.full((link_count, owners), BIG, jnp.int32)
        two = jnp.full((link_count, owners), -1, jnp.int32)
        for t in range(tiles):
            hit = (mine[t] == last) & (last < BIG)
            one = jnp.minimum(one, jnp.where(hit, link + t * link_count, BIG))
            two = jnp.maximum(two, jnp.where(hit, link + t * link_count, -1))
        one = jnp.min(one, axis=0, keepdims=True)
        two = jnp.max(two, axis=0, keepdims=True)
        for i in range(domains):
            link_one[i * per_owner + j] = one[0, i]
            link_two[i * per_owner + j] = two[0, i]

    acc[...] = jnp.zeros_like(acc)

    def product(sources, offsets=None):
        rimmed = offsets is not None
        totals = [acc[t] for t in range(tiles)]
        outer = [[0.0] * tiles for _ in range(per_owner)]
        for k, frm in enumerate(sources):
            for j in range(per_owner):
                here = buf[pl.ds(frm * planes + j * comps, comps)].astype(jnp.float32)
                lhs = here.reshape(count, cells)
                if rimmed:
                    rest = rim_in[offsets[k]].astype(jnp.float32)
                    rim = buf[frm * planes + full].astype(jnp.float32)
                    rim = jnp.where(core == 1, rim, rest)
                    lhs = jnp.concatenate([lhs, rim], axis=0)
                lhs = lhs.astype(jnp.bfloat16)
                one = link_one[frm * per_owner + j]
                two = link_two[frm * per_owner + j]
                at_one, at_two = jnp.minimum(one, links - 1), jnp.maximum(two, 0)
                quad = jnp.concatenate(
                    [w_ref[0, at_one], w_ref[1, at_one], w_ref[0, at_two], w_ref[1, at_two]],
                    axis=1,
                )
                both = jnp.dot(lhs, quad, preferred_element_type=jnp.float32)
                for t in range(tiles):
                    begin, end = t * link_count, (t + 1) * link_count
                    part = jnp.where(
                        (one >= begin) & (one < end), both[:, : 2 * width], 0.0
                    ) + jnp.where((two >= begin) & (two < end), both[:, 2 * width :], 0.0)
                    totals[t] += part[:count]
                    if rimmed:
                        outer[j][t] += part[count:]
        for t in range(tiles):
            acc[t] = totals[t]
            if rimmed:
                parts = [outer[j][t][j * comps : (j + 1) * comps] for j in range(per_owner)]
                rim_acc[t] += sum(parts)

    def arrive(box, number):
        rows_in = buf.at[pl.ds(0, number)]
        pltpu.make_async_remote_copy(
            src_ref=rows_in,
            dst_ref=rows_in,
            send_sem=send_sem,
            recv_sem=recv_sem.at[box],
            device_id=(me, other),
            device_id_type=mesh_type,
        ).wait_recv()

    def beyond_mid(i, apart):
        return me ^ (mid + i) ^ (quarter * apart)

    load_w.wait()
    swap_to(other).wait_recv()

    far, near = 1 - near_from, near_from
    outmost = jnp.where(plane == 0, 1, 0)

    def own_half(i):
        return me ^ (quarter + i)

    def far_half(i):
        return beyond_mid(i, far)

    def near_half(i):
        return beyond_mid(i, near)

    rim_acc[...] = jnp.zeros_like(rim_acc)
    halo = pltpu.make_async_remote_copy(
        src_ref=edge,
        dst_ref=beyond,
        send_sem=side_sem,
        recv_sem=edge_sem,
        device_id=(me, other),
        device_id_type=mesh_type,
    )

    def early_edge():
        now = acc[...].reshape(tiles, comps, half, 2 * width)
        edge[...] = jnp.where(core == 0, now[:, :, half - 1], now[:, :, 0])
        halo.start()

    if domains <= 16:
        product([me])
        arrive(0, (quarter - 1) * full)
        product([me ^ r for r in range(1, quarter)])
        arrive(1 + outmost, quarter * full)
        product([jnp.where(plane == 0, far_half(i), own_half(i)) for i in range(quarter)])
        arrive(2 - outmost, quarter * full)
        product([jnp.where(plane == 0, own_half(i), far_half(i)) for i in range(quarter)])
        early_edge()
    else:
        arrive(0, (quarter - 1) * full)
        arrive(1, quarter * full)
        arrive(2, quarter * full)
        steps(mid, lambda r: product([me ^ r]))
        steps(quarter, lambda i: product([far_half(i)]))
        early_edge()

    def arrive_near(offset):
        @pl.when(core == 0)
        def _():
            arrive(3 + offset, full)

        @pl.when(core == 1)
        def _():
            arrive(3 + offset, planes)

    def offset_of(i):
        by_column = lower * other
        return by_column * (i ^ (me % quarter)) + (1 - by_column) * (quarter - 1 - i)

    def handed(base):
        return pltpu.make_async_remote_copy(
            src_ref=rim_out.at[pl.ds(base, 2)],
            dst_ref=rim_in.at[pl.ds(base, 2)],
            send_sem=side_sem,
            recv_sem=rim_sem.at[base // 2],
            device_id=(me, other),
            device_id_type=mesh_type,
        )

    def hand(offset):
        frm, lines = near_half(offset), []
        for j in range(per_owner):
            block = buf[pl.ds(frm * planes + j * comps, comps)].astype(jnp.float32)
            lines.append(block[:, 0])
        if half > full:
            lines.append(jnp.zeros((half - full, cells), jnp.float32))
        rim_out[offset] = jnp.concatenate(lines, axis=0).astype(jnp.bfloat16)

    def late(i):
        pair = [offset_of(i), offset_of(i + 1)]
        base = pair[0] // 2 * 2
        for offset in pair:
            arrive_near(offset)

        @pl.when(core == 1)
        def _():
            for offset in pair:
                hand(offset)
            handed(base).start()

        pl.when(core == 0)(handed(base).wait_recv)
        product([near_half(offset) for offset in pair], pair)

    steps(quarter // 2, lambda i: late(2 * i))

    total = acc[...].reshape(tiles, comps, half, 2 * width)

    out_ref[0] = total.astype(jnp.bfloat16)

    def drain(number):
        sent = pack.at[pl.ds(0, number)]
        pltpu.make_async_remote_copy(
            src_ref=sent,
            dst_ref=sent,
            send_sem=send_sem,
            recv_sem=recv_sem.at[0],
            device_id=(me, other),
            device_id_type=mesh_type,
        ).wait_send()

    @pl.when(takes)
    def _():
        drain((domains - 1) * full + mid)

    @pl.when(jnp.logical_not(takes))
    def _():
        drain((domains - 1) * full)

    halo.wait_recv()
    sample = lax.broadcasted_iota(jnp.int32, (half, 2 * width), 0)
    for t in range(tiles):
        past = beyond[t] + rim_acc[t]
        for p in range(comps):
            now = total[t, p]
            outer = jnp.broadcast_to(past[p : p + 1], now.shape)
            later = pltpu.roll(now, half - 1, 0)
            prior = pltpu.roll(now, 1, 0)
            later = jnp.where((sample == half - 1) & (core == 0), outer, later)
            prior = jnp.where((sample == 0) & (core == 1), outer, prior)
            rate = jnp.where(
                (sample == 0) & (core == 0),
                later - now,
                jnp.where(
                    (sample == half - 1) & (core == 1), now - prior, (later - prior) * 0.5
                ),
            )
            out_ref[1, t, p] = rate.astype(jnp.bfloat16)
    swap.wait_send()
    pl.when(gives)(twin.wait_send)
    halo.wait_send()

    @pl.when(core == 1)
    def _():
        steps(quarter // 2, lambda i: handed(2 * i).wait_send())


def deliver(both_ref, source_ref, rate_ref, sem):
    copies = [
        pltpu.make_async_copy(both_ref.at[i], out, sem.at[i])
        for i, out in enumerate((source_ref, rate_ref))
    ]
    for copy in copies:
        copy.start()
    for copy in copies:
        copy.wait()


def shards(sources, weights, intersect, block_row, slot_tile):
    domains = lax.axis_size("dom")
    tiles, link_count, cells, width = weights.shape
    blocks, comps, half, _ = sources.shape
    links = tiles * link_count
    pool = links // 2
    per_owner = (pool + domains - 1) // domains
    vmem, smem = pltpu.VMEM, pltpu.SMEM
    shape = (tiles, comps, half, 2 * width)
    out = jax.ShapeDtypeStruct(shape, jnp.bfloat16)
    block = (half, cells)
    planes = per_owner * comps + 1
    dma, regular = pltpu.SemaphoreType.DMA, pltpu.SemaphoreType.REGULAR
    in_vmem = pl.BlockSpec(memory_space=vmem)
    anywhere = pl.BlockSpec(memory_space=pl.ANY)

    def wide(n):
        return vmem((link_count, -(-n // LANES) * LANES), jnp.int32)

    both = pl.pallas_call(
        functools.partial(kernel, domains, per_owner),
        out_shape=vmem((2,) + shape, jnp.bfloat16),
        in_specs=[anywhere] * 5,
        out_specs=in_vmem,
        scratch_shapes=[
            vmem((1, slot_tile.shape[0]), jnp.int32),
            vmem((1, block_row.shape[0]), jnp.int32),
            vmem((link_count, intersect.shape[0]), jnp.int32),
            vmem(sources.shape, jnp.bfloat16),
            wide(slot_tile.shape[0]),
            wide(block_row.shape[0]),
            wide(intersect.shape[0]),
            smem((domains * per_owner,), jnp.int32),
            smem((domains * per_owner,), jnp.int32),
            smem((domains * per_owner,), jnp.int32),
            vmem((2, links, cells, width), jnp.bfloat16),
            vmem((domains * planes,) + block, jnp.bfloat16),
            vmem((domains * planes,) + block, jnp.bfloat16),
            vmem((tiles, comps * half, 2 * width), jnp.float32),
            vmem((tiles, comps, 2 * width), jnp.float32),
            vmem((tiles, comps, 2 * width), jnp.float32),
            vmem(sources.shape, jnp.bfloat16),
            vmem((tiles, comps, 2 * width), jnp.float32),
            vmem((domains // 4,) + block, jnp.bfloat16),
            vmem((domains // 4,) + block, jnp.bfloat16),
            dma((2,)),
            dma,
            dma,
            dma((3 + domains // 4,)),
            dma,
            dma,
            dma,
            regular((domains // 4 + 1,)),
            regular,
            dma,
            dma((domains // 8,)),
        ],
        compiler_params=pltpu.CompilerParams(collective_id=0, has_side_effects=True),
        cost_estimate=pl.CostEstimate(
            flops=4 * comps * half * weights.size,
            bytes_accessed=2 * weights.size,
            transcendentals=0,
        ),
    )(
        slot_tile.reshape(1, -1),
        block_row.reshape(1, -1),
        intersect.T,
        sources,
        weights.reshape(links, cells, width),
    )
    return pl.pallas_call(
        deliver,
        out_shape=(out, out),
        in_specs=[in_vmem],
        out_specs=(anywhere, anywhere),
        scratch_shapes=[dma((2,))],
    )(pltpu.with_memory_space_constraint(both, vmem))


def solution(mesh):
    return jax.shard_map(
        shards,
        mesh=mesh,
        in_specs=(P("dom", None, "tm", None), P("dom", None, None, "tm"), P(), P(), P()),
        out_specs=(P("dom", None, "tm", None), P("dom", None, "tm", None)),
        check_vma=False,
    )
```

```python
import functools

import jax
import jax.numpy as jnp
from jax import lax
from jax.experimental import pallas as pl
from jax.experimental.pallas import tpu as pltpu
from jax.sharding import PartitionSpec as P


BIG = 1 << 30
LANES = 128


def lookup(table, index):
    within, group = index & (LANES - 1), index >> 7
    outs = []
    for at in range(0, index.shape[1], LANES):
        value = jnp.zeros((index.shape[0], LANES), jnp.int32)
        for g in range(table.shape[1] // LANES):
            got = jnp.take_along_axis(
                table[:, g * LANES : (g + 1) * LANES],
                within[:, at : at + LANES],
                axis=1,
                mode="promise_in_bounds",
            )
            value = jnp.where(group[:, at : at + LANES] == g, got, value)
        outs.append(value)
    return outs[0] if len(outs) == 1 else jnp.concatenate(outs, axis=1)


def steps(count, body):
    if count <= 16:
        for i in range(count):
            body(i)
    else:
        def step(i, carry):
            body(i)
            return carry
        lax.fori_loop(0, count, step, 0)


def kernel(
    domains, per_owner,
    tile_hbm, row_hbm, cross_hbm, src_hbm, w_hbm, out_ref,
    tile_ref, row_ref, cross_ref, src_ref,
    wide_tile, wide_row, wide_cross, send_to, link_one, link_two,
    w_ref, pack, buf, acc, edge, beyond, twin_ref, rim_acc, rim_out, rim_in,
    in_sem, w_sem, send_sem, recv_sem, side_sem, wrecv_sem, edge_sem, flag_sem, near_sem,
    twin_sem, rim_sem,
):
    me = lax.axis_index("dom")
    core = lax.axis_index("tm")
    other = 1 - core
    links, width = w_ref.shape[1], w_ref.shape[3]
    blocks, comps, half, cells = src_ref.shape
    tiles = acc.shape[0]
    link_count = links // tiles
    count = comps * half
    full = per_owner * comps
    planes = full + 1
    mesh_type = pl.DeviceIdType.MESH
    mid, quarter = domains // 2, domains // 4
    upper = me // mid
    lower = 1 - upper
    plane = me // quarter
    inner = (plane + 1) // 2 % 2 * quarter
    even = (1 - plane % 2) * quarter

    def key(d):
        hops = d % 2 + d // 2 % 2 + d // quarter
        shift = (0, 0, -1, 4)
        moved = sum(shift[p] * (d // quarter == p) for p in range(4))
        return (4 * hops + moved) * domains + d

    def wait_if(condition, sem, value):
        @pl.when(condition)
        def _():
            pl.semaphore_wait(sem, value)

    near_from = inner // quarter

    def mailbox(offset):
        return 2 + near_from * (1 + offset)

    inputs = [
        pltpu.make_async_copy(source, target, in_sem.at[i // 3])
        for i, (source, target) in enumerate(
            (
                (tile_hbm, tile_ref),
                (cross_hbm, cross_ref),
                (row_hbm, row_ref),
                (src_hbm, src_ref),
            )
        )
    ]
    for load in inputs:
        load.start()

    barrier = pltpu.get_barrier_semaphore()
    pl.semaphore_signal(barrier, inc=1, device_id=(me, other), device_id_type=mesh_type)

    def greet(i):
        to = domains - 1 - i

        @pl.when(key(to) > key(me))
        def _():
            pl.semaphore_signal(barrier, inc=1, device_id=(to, core), device_id_type=mesh_type)

    steps(domains, greet)

    load_w = pltpu.make_async_copy(w_hbm, w_ref.at[core], w_sem)
    load_w.start()

    wide_tile[...] = jnp.zeros_like(wide_tile)
    wide_cross[...] = jnp.zeros_like(wide_cross)
    wide_row[...] = jnp.zeros_like(wide_row)

    def swap_to(part):
        return pltpu.make_async_remote_copy(
            src_ref=w_hbm,
            dst_ref=w_ref.at[part],
            send_sem=side_sem,
            recv_sem=wrecv_sem,
            device_id=(me, other),
            device_id_type=mesh_type,
        )

    swap = swap_to(core)
    twin = pltpu.make_async_remote_copy(
        src_ref=src_hbm,
        dst_ref=twin_ref,
        send_sem=side_sem,
        recv_sem=twin_sem,
        device_id=(me, other),
        device_id_type=mesh_type,
    )
    gives = (core == 0) & (near_from == 1)
    takes = (core == 1) & (near_from == 1)
    def below(start, number):
        return sum((key(start + i) < key(me)).astype(jnp.int32) for i in range(number))

    before, near_before = below(0, domains), below(upper * mid, mid)

    flag = me % quarter + plane % 2 * (quarter - me % quarter)

    def announce(i):
        known = key(i) < key(me)

        @pl.when(known & (i // mid == upper))
        def _():
            pl.semaphore_signal(near_sem, inc=1, device_id=(i, core), device_id_type=mesh_type)

        @pl.when(known & (i // mid != upper))
        def _():
            pl.semaphore_signal(
                flag_sem.at[flag], inc=1, device_id=(i, core), device_id_type=mesh_type
            )

    for load in inputs[:3]:
        load.wait()
    wide_tile[:, : tile_ref.shape[1]] = jnp.broadcast_to(
        tile_ref[...], (link_count, tile_ref.shape[1])
    )
    wide_cross[:, : cross_ref.shape[1]] = cross_ref[...]
    wide_row[:, : row_ref.shape[1]] = jnp.broadcast_to(
        row_ref[...], (link_count, row_ref.shape[1])
    )
    owners = -(-domains // LANES) * LANES
    around = lax.broadcasted_iota(jnp.int32, (1, owners), 1)
    lane = lax.broadcasted_iota(jnp.int32, (link_count, owners), 1)
    named = lookup(wide_row[...], wide_cross[...])
    rows = []
    for t in range(tiles):
        slot = jnp.minimum(lane * tiles + t, tile_ref.shape[1] - 1)
        rows.append(lookup(named, lookup(wide_tile[...], slot)))

    base = me * blocks
    locals_ = [
        jnp.where((row >= base) & (row < base + blocks), row - base, BIG) for row in rows
    ]
    last = jnp.full((1, owners), -1, jnp.int32)
    for j in range(per_owner):
        left = [jnp.where(at > last, at, BIG) for at in locals_]
        last = jnp.min(functools.reduce(jnp.minimum, left), axis=0, keepdims=True)
        index = jnp.minimum(last, blocks - 1)
        for d in range(domains):
            send_to[d * per_owner + j] = index[0, d]

    def fill(d):
        for j in range(per_owner):
            pack[pl.ds(d * planes + j * comps, comps)] = src_ref[send_to[d * per_owner + j]]

    inputs[3].wait()
    steps(domains, fill)
    for j in range(per_owner):
        buf[pl.ds(me * planes + j * comps, comps)] = src_ref[send_to[me * per_owner + j]]

    def exchange(to, box, start=0, number=full):
        return pltpu.make_async_remote_copy(
            src_ref=pack.at[pl.ds(to * planes + start, number)],
            dst_ref=buf.at[pl.ds(me * planes + start, number)],
            send_sem=send_sem,
            recv_sem=recv_sem.at[box],
            device_id=(to, core),
            device_id_type=mesh_type,
        )

    def across(to, **part):
        exchange(to, mailbox((me ^ to) % quarter), **part).start()

    def first_of(i):
        to = me ^ (domains - 1 - i) ^ even
        return jnp.where(plane == 3, to, lower * mid + i)

    def first(i, **part):
        to = first_of(i)
        wait_if(key(to) > key(me), flag_sem.at[to % quarter], 1)
        across(to, **part)

    def second(i, **part):
        across(me ^ (mid + quarter - 1 - i) ^ even, **part)

    def beside(known):
        def send(i):
            r = mid - 1 - i
            to = me ^ r

            @pl.when((key(to) < key(me)) == known)
            def _():
                exchange(to, r // quarter).start()

        if domains <= 16:
            steps(mid - 1, send)
        else:
            steps(quarter, send)
            steps(quarter - 1, lambda i: send(i + quarter))

    pl.semaphore_wait(barrier, 1 + before)
    steps(domains, announce)
    pl.when(gives)(twin.start)
    swap.start()
    def rim_of(i):
        to, lines = lower * mid + i, []
        for j in range(per_owner):
            block = twin_ref[send_to[to * per_owner + j]].astype(jnp.float32)
            lines.append(block[:, half - 1])
        if half > full:
            lines.append(jnp.zeros((half - full, cells), jnp.float32))
        pack[to * planes + full] = jnp.concatenate(lines, axis=0).astype(jnp.bfloat16)

    def rim_alone(i):
        to = first_of(i)

        @pl.when(to > 0)
        def _():
            across(to, start=full, number=1)

    early = quarter - 1

    def fork(send, start, number):
        @pl.when(takes)
        def _():
            steps(number, lambda i: send(i + start, number=planes))

        @pl.when(jnp.logical_not(takes))
        def _():
            steps(number, lambda i: send(i + start))

    pl.when(upper == 0)(lambda: beside(True))
    steps(early, first)

    @pl.when(takes)
    def _():
        twin.wait_recv()
        steps(mid, rim_of)
        steps(early, rim_alone)

    fork(first, early, quarter - early)

    later = lower * mid + quarter
    due = quarter - below(later, quarter)

    @pl.when(upper == 1)
    def _():
        wait_if(due > 0, flag_sem.at[quarter], due)
        fork(second, 0, quarter)
        beside(True)

    wait_if(near_before < mid - 1, near_sem, mid - 1 - near_before)
    beside(False)

    @pl.when(upper == 0)
    def _():
        pl.semaphore_wait(flag_sem.at[quarter], due)
        fork(second, 0, quarter)


    link = lax.broadcasted_iota(jnp.int32, (link_count, owners), 0)
    mine = []
    for t in range(tiles):
        column = jnp.sum(jnp.where(lane == me, rows[t], 0), axis=1, keepdims=True)
        at = column - around * blocks
        mine.append(jnp.where((at >= 0) & (at < blocks), at, BIG))
    last = jnp.full((1, owners), -1, jnp.int32)
    for j in range(per_owner):
        least = [jnp.where(at > last, at, BIG) for at in mine]
        last = jnp.min(functools.reduce(jnp.minimum, least), axis=0, keepdims=True)
        one = jnp.full((link_count, owners), BIG, jnp.int32)
        two = jnp.full((link_count, owners), -1, jnp.int32)
        for t in range(tiles):
            hit = (mine[t] == last) & (last < BIG)
            one = jnp.minimum(one, jnp.where(hit, link + t * link_count, BIG))
            two = jnp.maximum(two, jnp.where(hit, link + t * link_count, -1))
        one = jnp.min(one, axis=0, keepdims=True)
        two = jnp.max(two, axis=0, keepdims=True)
        for i in range(domains):
            link_one[i * per_owner + j] = one[0, i]
            link_two[i * per_owner + j] = two[0, i]

    acc[...] = jnp.zeros_like(acc)

    def product(sources, offsets=None):
        rimmed = offsets is not None
        totals = [acc[t] for t in range(tiles)]
        outer = [[0.0] * tiles for _ in range(per_owner)]
        for k, frm in enumerate(sources):
            for j in range(per_owner):
                here = buf[pl.ds(frm * planes + j * comps, comps)].astype(jnp.float32)
                lhs = here.reshape(count, cells)
                if rimmed:
                    rest = rim_in[offsets[k]].astype(jnp.float32)
                    rim = buf[frm * planes + full].astype(jnp.float32)
                    rim = jnp.where(core == 0, rest, jnp.where(me == 0, 0.0, rim))
                    lhs = jnp.concatenate([lhs, rim], axis=0)
                lhs = lhs.astype(jnp.bfloat16)
                one = link_one[frm * per_owner + j]
                two = link_two[frm * per_owner + j]
                at_one, at_two = jnp.minimum(one, links - 1), jnp.maximum(two, 0)
                quad = jnp.concatenate(
                    [w_ref[0, at_one], w_ref[1, at_one], w_ref[0, at_two], w_ref[1, at_two]],
                    axis=1,
                )
                both = jnp.dot(lhs, quad, preferred_element_type=jnp.float32)
                for t in range(tiles):
                    begin, end = t * link_count, (t + 1) * link_count
                    part = jnp.where(
                        (one >= begin) & (one < end), both[:, : 2 * width], 0.0
                    ) + jnp.where((two >= begin) & (two < end), both[:, 2 * width :], 0.0)
                    totals[t] += part[:count]
                    if rimmed:
                        outer[j][t] += part[count:]
        for t in range(tiles):
            acc[t] = totals[t]
            if rimmed:
                parts = [outer[j][t][j * comps : (j + 1) * comps] for j in range(per_owner)]
                rim_acc[t] += sum(parts)

    def arrive(box, number):
        rows_in = buf.at[pl.ds(0, number)]
        pltpu.make_async_remote_copy(
            src_ref=rows_in,
            dst_ref=rows_in,
            send_sem=send_sem,
            recv_sem=recv_sem.at[box],
            device_id=(me, other),
            device_id_type=mesh_type,
        ).wait_recv()

    def beyond_mid(i, apart):
        return me ^ (mid + i) ^ (quarter * apart)

    load_w.wait()
    swap_to(other).wait_recv()

    far, near = 1 - near_from, near_from
    outmost = jnp.where(plane == 0, 1, 0)

    def own_half(i):
        return me ^ (quarter + i)

    def far_half(i):
        return beyond_mid(i, far)

    def near_half(i):
        return beyond_mid(i, near)

    rim_acc[...] = jnp.zeros_like(rim_acc)
    halo = pltpu.make_async_remote_copy(
        src_ref=edge,
        dst_ref=beyond,
        send_sem=side_sem,
        recv_sem=edge_sem,
        device_id=(me, other),
        device_id_type=mesh_type,
    )

    tardy = (core == 0) & (me == 0)

    def give_edge():
        now = acc[...].reshape(tiles, comps, half, 2 * width)
        edge[...] = jnp.where(core == 0, now[:, :, half - 1], now[:, :, 0])
        halo.start()

    if domains <= 16:
        product([me])
        arrive(0, (quarter - 1) * full)
        product([me ^ r for r in range(1, quarter)])
        arrive(1 + outmost, quarter * full)
        product([jnp.where(plane == 0, far_half(i), own_half(i)) for i in range(quarter)])
        arrive(2 - outmost, quarter * full)
        product([jnp.where(plane == 0, own_half(i), far_half(i)) for i in range(quarter)])
        pl.when(jnp.logical_not(tardy))(give_edge)
    else:
        arrive(0, (quarter - 1) * full)
        arrive(1, quarter * full)
        arrive(2, quarter * full)
        steps(mid, lambda r: product([me ^ r]))
        steps(quarter, lambda i: product([far_half(i)]))
        pl.when(jnp.logical_not(tardy))(give_edge)

    bare = (core == 0) | (me == 0)

    def arrive_near(offset):
        @pl.when(bare)
        def _():
            arrive(3 + offset, full)

        @pl.when(jnp.logical_not(bare))
        def _():
            arrive(3 + offset, planes)

    def offset_of(i):
        by_column = lower * other
        return by_column * (i ^ (me % quarter)) + (1 - by_column) * (quarter - 1 - i)

    def handed(base):
        return pltpu.make_async_remote_copy(
            src_ref=rim_out.at[pl.ds(base, 2)],
            dst_ref=rim_in.at[pl.ds(base, 2)],
            send_sem=side_sem,
            recv_sem=rim_sem.at[base // 2],
            device_id=(me, other),
            device_id_type=mesh_type,
        )

    def hand(offset):
        frm, lines = near_half(offset), []
        for j in range(per_owner):
            block = buf[pl.ds(frm * planes + j * comps, comps)].astype(jnp.float32)
            lines.append(block[:, 0])
        if half > full:
            lines.append(jnp.zeros((half - full, cells), jnp.float32))
        rim_out[offset] = jnp.concatenate(lines, axis=0).astype(jnp.bfloat16)

    def late(i):
        pair = [offset_of(i), offset_of(i + 1)]
        base = pair[0] // 2 * 2
        for offset in pair:
            arrive_near(offset)

        @pl.when(core == 1)
        def _():
            for offset in pair:
                hand(offset)
            handed(base).start()

        pl.when(core == 0)(handed(base).wait_recv)
        product([near_half(offset) for offset in pair], pair)

    steps(quarter // 2, lambda i: late(2 * i))
    pl.when(tardy)(give_edge)

    total = acc[...].reshape(tiles, comps, half, 2 * width)

    out_ref[0] = total.astype(jnp.bfloat16)

    def drain(number):
        sent = pack.at[pl.ds(0, number)]
        pltpu.make_async_remote_copy(
            src_ref=sent,
            dst_ref=sent,
            send_sem=send_sem,
            recv_sem=recv_sem.at[0],
            device_id=(me, other),
            device_id_type=mesh_type,
        ).wait_send()

    @pl.when(takes & (plane == 1))
    def _():
        drain((domains - 1) * full + mid)

    @pl.when(takes & (plane == 2))
    def _():
        drain((domains - 1) * full + mid - 1)

    @pl.when(jnp.logical_not(takes))
    def _():
        drain((domains - 1) * full)

    halo.wait_recv()
    sample = lax.broadcasted_iota(jnp.int32, (half, 2 * width), 0)
    for t in range(tiles):
        past = beyond[t] + rim_acc[t]
        for p in range(comps):
            now = total[t, p]
            outer = jnp.broadcast_to(past[p : p + 1], now.shape)
            later = pltpu.roll(now, half - 1, 0)
            prior = pltpu.roll(now, 1, 0)
            later = jnp.where((sample == half - 1) & (core == 0), outer, later)
            prior = jnp.where((sample == 0) & (core == 1), outer, prior)
            rate = jnp.where(
                (sample == 0) & (core == 0),
                later - now,
                jnp.where(
                    (sample == half - 1) & (core == 1), now - prior, (later - prior) * 0.5
                ),
            )
            out_ref[1, t, p] = rate.astype(jnp.bfloat16)
    swap.wait_send()
    pl.when(gives)(twin.wait_send)
    halo.wait_send()

    @pl.when(core == 1)
    def _():
        steps(quarter // 2, lambda i: handed(2 * i).wait_send())


def deliver(both_ref, source_ref, rate_ref, sem):
    copies = [
        pltpu.make_async_copy(both_ref.at[i], out, sem.at[i])
        for i, out in enumerate((source_ref, rate_ref))
    ]
    for copy in copies:
        copy.start()
    for copy in copies:
        copy.wait()


def shards(sources, weights, intersect, block_row, slot_tile):
    domains = lax.axis_size("dom")
    tiles, link_count, cells, width = weights.shape
    blocks, comps, half, _ = sources.shape
    links = tiles * link_count
    pool = links // 2
    per_owner = (pool + domains - 1) // domains
    vmem, smem = pltpu.VMEM, pltpu.SMEM
    shape = (tiles, comps, half, 2 * width)
    out = jax.ShapeDtypeStruct(shape, jnp.bfloat16)
    block = (half, cells)
    planes = per_owner * comps + 1
    dma, regular = pltpu.SemaphoreType.DMA, pltpu.SemaphoreType.REGULAR
    in_vmem = pl.BlockSpec(memory_space=vmem)
    anywhere = pl.BlockSpec(memory_space=pl.ANY)

    def wide(n):
        return vmem((link_count, -(-n // LANES) * LANES), jnp.int32)

    both = pl.pallas_call(
        functools.partial(kernel, domains, per_owner),
        out_shape=vmem((2,) + shape, jnp.bfloat16),
        in_specs=[anywhere] * 5,
        out_specs=in_vmem,
        scratch_shapes=[
            vmem((1, slot_tile.shape[0]), jnp.int32),
            vmem((1, block_row.shape[0]), jnp.int32),
            vmem((link_count, intersect.shape[0]), jnp.int32),
            vmem(sources.shape, jnp.bfloat16),
            wide(slot_tile.shape[0]),
            wide(block_row.shape[0]),
            wide(intersect.shape[0]),
            smem((domains * per_owner,), jnp.int32),
            smem((domains * per_owner,), jnp.int32),
            smem((domains * per_owner,), jnp.int32),
            vmem((2, links, cells, width), jnp.bfloat16),
            vmem((domains * planes,) + block, jnp.bfloat16),
            vmem((domains * planes,) + block, jnp.bfloat16),
            vmem((tiles, comps * half, 2 * width), jnp.float32),
            vmem((tiles, comps, 2 * width), jnp.float32),
            vmem((tiles, comps, 2 * width), jnp.float32),
            vmem(sources.shape, jnp.bfloat16),
            vmem((tiles, comps, 2 * width), jnp.float32),
            vmem((domains // 4,) + block, jnp.bfloat16),
            vmem((domains // 4,) + block, jnp.bfloat16),
            dma((2,)),
            dma,
            dma,
            dma((3 + domains // 4,)),
            dma,
            dma,
            dma,
            regular((domains // 4 + 1,)),
            regular,
            dma,
            dma((domains // 8,)),
        ],
        compiler_params=pltpu.CompilerParams(collective_id=0, has_side_effects=True),
        cost_estimate=pl.CostEstimate(
            flops=4 * comps * half * weights.size,
            bytes_accessed=2 * weights.size,
            transcendentals=0,
        ),
    )(
        slot_tile.reshape(1, -1),
        block_row.reshape(1, -1),
        intersect.T,
        sources,
        weights.reshape(links, cells, width),
    )
    return pl.pallas_call(
        deliver,
        out_shape=(out, out),
        in_specs=[in_vmem],
        out_specs=(anywhere, anywhere),
        scratch_shapes=[dma((2,))],
    )(pltpu.with_memory_space_constraint(both, vmem))


def solution(mesh):
    return jax.shard_map(
        shards,
        mesh=mesh,
        in_specs=(P("dom", None, "tm", None), P("dom", None, None, "tm"), P(), P(), P()),
        out_specs=(P("dom", None, "tm", None), P("dom", None, "tm", None)),
        check_vma=False,
    )
```

```python
import functools

import jax
import jax.numpy as jnp
from jax import lax
from jax.experimental import pallas as pl
from jax.experimental.pallas import tpu as pltpu
from jax.sharding import PartitionSpec as P


BIG = 1 << 30
LANES = 128


def lookup(table, index):
    within, group = index & (LANES - 1), index >> 7
    outs = []
    for at in range(0, index.shape[1], LANES):
        value = jnp.zeros((index.shape[0], LANES), jnp.int32)
        for g in range(table.shape[1] // LANES):
            got = jnp.take_along_axis(
                table[:, g * LANES : (g + 1) * LANES],
                within[:, at : at + LANES],
                axis=1,
                mode="promise_in_bounds",
            )
            value = jnp.where(group[:, at : at + LANES] == g, got, value)
        outs.append(value)
    return outs[0] if len(outs) == 1 else jnp.concatenate(outs, axis=1)


def steps(count, body):
    if count <= 16:
        for i in range(count):
            body(i)
    else:
        def step(i, carry):
            body(i)
            return carry
        lax.fori_loop(0, count, step, 0)


def kernel(
    domains, per_owner,
    tile_hbm, row_hbm, cross_hbm, src_hbm, w_hbm, out_ref,
    tile_ref, row_ref, cross_ref, src_ref,
    wide_tile, wide_row, wide_cross, send_to, link_one, link_two,
    w_ref, pack, buf, acc, edge, beyond, twin_ref, rim_acc, rim_out, rim_in,
    in_sem, w_sem, send_sem, recv_sem, side_sem, wrecv_sem, edge_sem, flag_sem, near_sem,
    twin_sem, rim_sem,
):
    me = lax.axis_index("dom")
    core = lax.axis_index("tm")
    other = 1 - core
    links, width = w_ref.shape[1], w_ref.shape[3]
    blocks, comps, half, cells = src_ref.shape
    tiles = acc.shape[0]
    link_count = links // tiles
    count = comps * half
    full = per_owner * comps
    planes = full + 1
    mesh_type = pl.DeviceIdType.MESH
    mid, quarter = domains // 2, domains // 4
    upper = me // mid
    lower = 1 - upper
    plane = me // quarter
    inner = (plane + 1) // 2 % 2 * quarter
    even = (1 - plane % 2) * quarter

    def key(d):
        hops = d % 2 + d // 2 % 2 + d // quarter
        shift = (0, 0, -1, 4)
        moved = sum(shift[p] * (d // quarter == p) for p in range(4))
        return (4 * hops + moved) * domains + d

    def wait_if(condition, sem, value):
        @pl.when(condition)
        def _():
            pl.semaphore_wait(sem, value)

    near_from = inner // quarter

    def mailbox(offset):
        return 2 + near_from * (1 + offset)

    inputs = [
        pltpu.make_async_copy(source, target, in_sem.at[i // 3])
        for i, (source, target) in enumerate(
            (
                (tile_hbm, tile_ref),
                (cross_hbm, cross_ref),
                (row_hbm, row_ref),
                (src_hbm, src_ref),
            )
        )
    ]
    for load in inputs:
        load.start()

    barrier = pltpu.get_barrier_semaphore()
    pl.semaphore_signal(barrier, inc=1, device_id=(me, other), device_id_type=mesh_type)

    def greet(i):
        to = domains - 1 - i

        @pl.when(key(to) > key(me))
        def _():
            pl.semaphore_signal(barrier, inc=1, device_id=(to, core), device_id_type=mesh_type)

    steps(domains, greet)

    load_w = pltpu.make_async_copy(w_hbm, w_ref.at[core], w_sem)
    load_w.start()

    wide_tile[...] = jnp.zeros_like(wide_tile)
    wide_cross[...] = jnp.zeros_like(wide_cross)
    wide_row[...] = jnp.zeros_like(wide_row)

    def swap_to(part):
        return pltpu.make_async_remote_copy(
            src_ref=w_hbm,
            dst_ref=w_ref.at[part],
            send_sem=side_sem,
            recv_sem=wrecv_sem,
            device_id=(me, other),
            device_id_type=mesh_type,
        )

    swap = swap_to(core)
    twin = pltpu.make_async_remote_copy(
        src_ref=src_hbm,
        dst_ref=twin_ref,
        send_sem=side_sem,
        recv_sem=twin_sem,
        device_id=(me, other),
        device_id_type=mesh_type,
    )
    gives = (core == 0) & (near_from == 1)
    takes = (core == 1) & (near_from == 1)
    def below(start, number):
        return sum((key(start + i) < key(me)).astype(jnp.int32) for i in range(number))

    before, near_before = below(0, domains), below(upper * mid, mid)

    flag = me % quarter + plane % 2 * (quarter - me % quarter)

    def announce(i):
        known = key(i) < key(me)

        @pl.when(known & (i // mid == upper))
        def _():
            pl.semaphore_signal(near_sem, inc=1, device_id=(i, core), device_id_type=mesh_type)

        @pl.when(known & (i // mid != upper))
        def _():
            pl.semaphore_signal(
                flag_sem.at[flag], inc=1, device_id=(i, core), device_id_type=mesh_type
            )

    for load in inputs[:3]:
        load.wait()
    wide_tile[:, : tile_ref.shape[1]] = jnp.broadcast_to(
        tile_ref[...], (link_count, tile_ref.shape[1])
    )
    wide_cross[:, : cross_ref.shape[1]] = cross_ref[...]
    wide_row[:, : row_ref.shape[1]] = jnp.broadcast_to(
        row_ref[...], (link_count, row_ref.shape[1])
    )
    owners = -(-domains // LANES) * LANES
    around = lax.broadcasted_iota(jnp.int32, (1, owners), 1)
    lane = lax.broadcasted_iota(jnp.int32, (link_count, owners), 1)
    named = lookup(wide_row[...], wide_cross[...])
    rows = []
    for t in range(tiles):
        slot = jnp.minimum(lane * tiles + t, tile_ref.shape[1] - 1)
        rows.append(lookup(named, lookup(wide_tile[...], slot)))

    base = me * blocks
    locals_ = [
        jnp.where((row >= base) & (row < base + blocks), row - base, BIG) for row in rows
    ]
    last = jnp.full((1, owners), -1, jnp.int32)
    for j in range(per_owner):
        left = [jnp.where(at > last, at, BIG) for at in locals_]
        last = jnp.min(functools.reduce(jnp.minimum, left), axis=0, keepdims=True)
        index = jnp.minimum(last, blocks - 1)
        for d in range(domains):
            send_to[d * per_owner + j] = index[0, d]

    def fill(d):
        for j in range(per_owner):
            pack[pl.ds(d * planes + j * comps, comps)] = src_ref[send_to[d * per_owner + j]]

    inputs[3].wait()
    steps(domains, fill)
    for j in range(per_owner):
        buf[pl.ds(me * planes + j * comps, comps)] = src_ref[send_to[me * per_owner + j]]

    def exchange(to, box, start=0, number=full):
        return pltpu.make_async_remote_copy(
            src_ref=pack.at[pl.ds(to * planes + start, number)],
            dst_ref=buf.at[pl.ds(me * planes + start, number)],
            send_sem=send_sem,
            recv_sem=recv_sem.at[box],
            device_id=(to, core),
            device_id_type=mesh_type,
        )

    def across(to, **part):
        exchange(to, mailbox((me ^ to) % quarter), **part).start()

    def first_of(i):
        to = me ^ (domains - 1 - i) ^ even
        return jnp.where(plane == 3, to, lower * mid + i)

    def first(i, **part):
        to = first_of(i)
        wait_if(key(to) > key(me), flag_sem.at[to % quarter], 1)
        across(to, **part)

    def second(i, **part):
        across(me ^ (mid + quarter - 1 - i) ^ even, **part)

    def beside(known):
        def send(i):
            r = mid - 1 - i
            to = me ^ r

            @pl.when((key(to) < key(me)) == known)
            def _():
                exchange(to, r // quarter).start()

        if domains <= 16:
            steps(mid - 1, send)
        else:
            steps(quarter, send)
            steps(quarter - 1, lambda i: send(i + quarter))

    pl.semaphore_wait(barrier, 1 + before)
    steps(domains, announce)
    pl.when(gives)(twin.start)
    swap.start()
    def rim_of(i):
        to, lines = lower * mid + i, []
        for j in range(per_owner):
            block = twin_ref[send_to[to * per_owner + j]].astype(jnp.float32)
            lines.append(block[:, half - 1])
        if half > full:
            lines.append(jnp.zeros((half - full, cells), jnp.float32))
        pack[to * planes + full] = jnp.concatenate(lines, axis=0).astype(jnp.bfloat16)

    def rim_alone(i):
        to = first_of(i)

        @pl.when(to > 0)
        def _():
            across(to, start=full, number=1)

    early = quarter - 1

    def fork(send, start, number):
        @pl.when(takes)
        def _():
            steps(number, lambda i: send(i + start, number=planes))

        @pl.when(jnp.logical_not(takes))
        def _():
            steps(number, lambda i: send(i + start))

    pl.when(upper == 0)(lambda: beside(True))
    steps(early, first)

    @pl.when(takes)
    def _():
        twin.wait_recv()
        steps(mid, rim_of)
        steps(early, rim_alone)

    fork(first, early, quarter - early)

    later = lower * mid + quarter
    due = quarter - below(later, quarter)

    @pl.when(upper == 1)
    def _():
        wait_if(due > 0, flag_sem.at[quarter], due)
        fork(second, 0, quarter)
        beside(True)

    wait_if(near_before < mid - 1, near_sem, mid - 1 - near_before)
    beside(False)

    @pl.when(upper == 0)
    def _():
        pl.semaphore_wait(flag_sem.at[quarter], due)
        fork(second, 0, quarter)


    link = lax.broadcasted_iota(jnp.int32, (link_count, owners), 0)
    mine = []
    for t in range(tiles):
        column = jnp.sum(jnp.where(lane == me, rows[t], 0), axis=1, keepdims=True)
        at = column - around * blocks
        mine.append(jnp.where((at >= 0) & (at < blocks), at, BIG))
    last = jnp.full((1, owners), -1, jnp.int32)
    for j in range(per_owner):
        least = [jnp.where(at > last, at, BIG) for at in mine]
        last = jnp.min(functools.reduce(jnp.minimum, least), axis=0, keepdims=True)
        one = jnp.full((link_count, owners), BIG, jnp.int32)
        two = jnp.full((link_count, owners), -1, jnp.int32)
        for t in range(tiles):
            hit = (mine[t] == last) & (last < BIG)
            one = jnp.minimum(one, jnp.where(hit, link + t * link_count, BIG))
            two = jnp.maximum(two, jnp.where(hit, link + t * link_count, -1))
        one = jnp.min(one, axis=0, keepdims=True)
        two = jnp.max(two, axis=0, keepdims=True)
        for i in range(domains):
            link_one[i * per_owner + j] = one[0, i]
            link_two[i * per_owner + j] = two[0, i]

    acc[...] = jnp.zeros_like(acc)

    def product(sources, offsets=None):
        rimmed = offsets is not None
        totals = [acc[t] for t in range(tiles)]
        outer = [[0.0] * tiles for _ in range(per_owner)]
        for k, frm in enumerate(sources):
            for j in range(per_owner):
                here = buf[pl.ds(frm * planes + j * comps, comps)].astype(jnp.float32)
                lhs = here.reshape(count, cells)
                if rimmed:
                    rest = rim_in[offsets[k]].astype(jnp.float32)
                    rim = buf[frm * planes + full].astype(jnp.float32)
                    rim = jnp.where(core == 0, rest, jnp.where(me == 0, 0.0, rim))
                    lhs = jnp.concatenate([lhs, rim], axis=0)
                lhs = lhs.astype(jnp.bfloat16)
                one = link_one[frm * per_owner + j]
                two = link_two[frm * per_owner + j]
                at_one, at_two = jnp.minimum(one, links - 1), jnp.maximum(two, 0)
                quad = jnp.concatenate(
                    [w_ref[0, at_one], w_ref[1, at_one], w_ref[0, at_two], w_ref[1, at_two]],
                    axis=1,
                )
                both = jnp.dot(lhs, quad, preferred_element_type=jnp.float32)
                for t in range(tiles):
                    begin, end = t * link_count, (t + 1) * link_count
                    part = jnp.where(
                        (one >= begin) & (one < end), both[:, : 2 * width], 0.0
                    ) + jnp.where((two >= begin) & (two < end), both[:, 2 * width :], 0.0)
                    totals[t] += part[:count]
                    if rimmed:
                        outer[j][t] += part[count:]
        for t in range(tiles):
            acc[t] = totals[t]
            if rimmed:
                parts = [outer[j][t][j * comps : (j + 1) * comps] for j in range(per_owner)]
                rim_acc[t] += sum(parts)

    def arrive(box, number):
        rows_in = buf.at[pl.ds(0, number)]
        pltpu.make_async_remote_copy(
            src_ref=rows_in,
            dst_ref=rows_in,
            send_sem=send_sem,
            recv_sem=recv_sem.at[box],
            device_id=(me, other),
            device_id_type=mesh_type,
        ).wait_recv()

    def beyond_mid(i, apart):
        return me ^ (mid + i) ^ (quarter * apart)

    load_w.wait()
    swap_to(other).wait_recv()

    far, near = 1 - near_from, near_from
    outmost = jnp.where(plane == 0, 1, 0)

    def own_half(i):
        return me ^ (quarter + i)

    def far_half(i):
        return beyond_mid(i, far)

    def near_half(i):
        return beyond_mid(i, near)

    rim_acc[...] = jnp.zeros_like(rim_acc)
    halo = pltpu.make_async_remote_copy(
        src_ref=edge,
        dst_ref=beyond,
        send_sem=side_sem,
        recv_sem=edge_sem,
        device_id=(me, other),
        device_id_type=mesh_type,
    )

    tardy = (core == 0) & (me == 0)

    def give_edge():
        now = acc[...].reshape(tiles, comps, half, 2 * width)
        edge[...] = jnp.where(core == 0, now[:, :, half - 1], now[:, :, 0])
        halo.start()

    if domains <= 16:
        product([me])
        arrive(0, (quarter - 1) * full)
        product([me ^ r for r in range(1, quarter)])
        arrive(1 + outmost, quarter * full)
        product([jnp.where(plane == 0, far_half(i), own_half(i)) for i in range(quarter)])
        arrive(2 - outmost, quarter * full)
        product([jnp.where(plane == 0, own_half(i), far_half(i)) for i in range(quarter)])
        pl.when(jnp.logical_not(tardy))(give_edge)
    else:
        arrive(0, (quarter - 1) * full)
        arrive(1, quarter * full)
        arrive(2, quarter * full)
        steps(mid, lambda r: product([me ^ r]))
        steps(quarter, lambda i: product([far_half(i)]))
        pl.when(jnp.logical_not(tardy))(give_edge)

    bare = (core == 0) | (me == 0)

    def arrive_near(offset):
        @pl.when(bare)
        def _():
            arrive(3 + offset, full)

        @pl.when(jnp.logical_not(bare))
        def _():
            arrive(3 + offset, planes)

    def offset_of(i):
        return quarter - 1 - i

    def handed(base):
        return pltpu.make_async_remote_copy(
            src_ref=rim_out.at[pl.ds(base, 2)],
            dst_ref=rim_in.at[pl.ds(base, 2)],
            send_sem=side_sem,
            recv_sem=rim_sem.at[base // 2],
            device_id=(me, other),
            device_id_type=mesh_type,
        )

    def hand(offset):
        frm, lines = near_half(offset), []
        for j in range(per_owner):
            block = buf[pl.ds(frm * planes + j * comps, comps)].astype(jnp.float32)
            lines.append(block[:, 0])
        if half > full:
            lines.append(jnp.zeros((half - full, cells), jnp.float32))
        rim_out[offset] = jnp.concatenate(lines, axis=0).astype(jnp.bfloat16)

    def late(i):
        pair = [offset_of(i), offset_of(i + 1)]
        base = pair[0] // 2 * 2
        for offset in pair:
            arrive_near(offset)

        @pl.when(core == 1)
        def _():
            for offset in pair:
                hand(offset)
            handed(base).start()

        pl.when(core == 0)(handed(base).wait_recv)
        product([near_half(offset) for offset in pair], pair)

    steps(quarter // 2, lambda i: late(2 * i))
    pl.when(tardy)(give_edge)

    total = acc[...].reshape(tiles, comps, half, 2 * width)

    out_ref[0] = total.astype(jnp.bfloat16)

    def drain(number):
        sent = pack.at[pl.ds(0, number)]
        pltpu.make_async_remote_copy(
            src_ref=sent,
            dst_ref=sent,
            send_sem=send_sem,
            recv_sem=recv_sem.at[0],
            device_id=(me, other),
            device_id_type=mesh_type,
        ).wait_send()

    @pl.when(takes & (plane == 1))
    def _():
        drain((domains - 1) * full + mid)

    @pl.when(takes & (plane == 2))
    def _():
        drain((domains - 1) * full + mid - 1)

    @pl.when(jnp.logical_not(takes))
    def _():
        drain((domains - 1) * full)

    halo.wait_recv()
    sample = lax.broadcasted_iota(jnp.int32, (half, 2 * width), 0)
    for t in range(tiles):
        past = beyond[t] + rim_acc[t]
        for p in range(comps):
            now = total[t, p]
            outer = jnp.broadcast_to(past[p : p + 1], now.shape)
            later = pltpu.roll(now, half - 1, 0)
            prior = pltpu.roll(now, 1, 0)
            later = jnp.where((sample == half - 1) & (core == 0), outer, later)
            prior = jnp.where((sample == 0) & (core == 1), outer, prior)
            rate = jnp.where(
                (sample == 0) & (core == 0),
                later - now,
                jnp.where(
                    (sample == half - 1) & (core == 1), now - prior, (later - prior) * 0.5
                ),
            )
            out_ref[1, t, p] = rate.astype(jnp.bfloat16)
    swap.wait_send()
    pl.when(gives)(twin.wait_send)
    halo.wait_send()

    @pl.when(core == 1)
    def _():
        steps(quarter // 2, lambda i: handed(2 * i).wait_send())


def deliver(both_ref, source_ref, rate_ref, sem):
    copies = [
        pltpu.make_async_copy(both_ref.at[i], out, sem.at[i])
        for i, out in enumerate((source_ref, rate_ref))
    ]
    for copy in copies:
        copy.start()
    for copy in copies:
        copy.wait()


def shards(sources, weights, intersect, block_row, slot_tile):
    domains = lax.axis_size("dom")
    tiles, link_count, cells, width = weights.shape
    blocks, comps, half, _ = sources.shape
    links = tiles * link_count
    pool = links // 2
    per_owner = (pool + domains - 1) // domains
    vmem, smem = pltpu.VMEM, pltpu.SMEM
    shape = (tiles, comps, half, 2 * width)
    out = jax.ShapeDtypeStruct(shape, jnp.bfloat16)
    block = (half, cells)
    planes = per_owner * comps + 1
    dma, regular = pltpu.SemaphoreType.DMA, pltpu.SemaphoreType.REGULAR
    in_vmem = pl.BlockSpec(memory_space=vmem)
    anywhere = pl.BlockSpec(memory_space=pl.ANY)

    def wide(n):
        return vmem((link_count, -(-n // LANES) * LANES), jnp.int32)

    both = pl.pallas_call(
        functools.partial(kernel, domains, per_owner),
        out_shape=vmem((2,) + shape, jnp.bfloat16),
        in_specs=[anywhere] * 5,
        out_specs=in_vmem,
        scratch_shapes=[
            vmem((1, slot_tile.shape[0]), jnp.int32),
            vmem((1, block_row.shape[0]), jnp.int32),
            vmem((link_count, intersect.shape[0]), jnp.int32),
            vmem(sources.shape, jnp.bfloat16),
            wide(slot_tile.shape[0]),
            wide(block_row.shape[0]),
            wide(intersect.shape[0]),
            smem((domains * per_owner,), jnp.int32),
            smem((domains * per_owner,), jnp.int32),
            smem((domains * per_owner,), jnp.int32),
            vmem((2, links, cells, width), jnp.bfloat16),
            vmem((domains * planes,) + block, jnp.bfloat16),
            vmem((domains * planes,) + block, jnp.bfloat16),
            vmem((tiles, comps * half, 2 * width), jnp.float32),
            vmem((tiles, comps, 2 * width), jnp.float32),
            vmem((tiles, comps, 2 * width), jnp.float32),
            vmem(sources.shape, jnp.bfloat16),
            vmem((tiles, comps, 2 * width), jnp.float32),
            vmem((domains // 4,) + block, jnp.bfloat16),
            vmem((domains // 4,) + block, jnp.bfloat16),
            dma((2,)),
            dma,
            dma,
            dma((3 + domains // 4,)),
            dma,
            dma,
            dma,
            regular((domains // 4 + 1,)),
            regular,
            dma,
            dma((domains // 8,)),
        ],
        compiler_params=pltpu.CompilerParams(collective_id=0, has_side_effects=True),
        cost_estimate=pl.CostEstimate(
            flops=4 * comps * half * weights.size,
            bytes_accessed=2 * weights.size,
            transcendentals=0,
        ),
    )(
        slot_tile.reshape(1, -1),
        block_row.reshape(1, -1),
        intersect.T,
        sources,
        weights.reshape(links, cells, width),
    )
    return pl.pallas_call(
        deliver,
        out_shape=(out, out),
        in_specs=[in_vmem],
        out_specs=(anywhere, anywhere),
        scratch_shapes=[dma((2,))],
    )(pltpu.with_memory_space_constraint(both, vmem))


def solution(mesh):
    return jax.shard_map(
        shards,
        mesh=mesh,
        in_specs=(P("dom", None, "tm", None), P("dom", None, None, "tm"), P(), P(), P()),
        out_specs=(P("dom", None, "tm", None), P("dom", None, "tm", None)),
        check_vma=False,
    )
```

```python
import functools

import jax
import jax.numpy as jnp
from jax import lax
from jax.experimental import pallas as pl
from jax.experimental.pallas import tpu as pltpu
from jax.sharding import PartitionSpec as P


BIG = 1 << 30
LANES = 128


def lookup(table, index):
    within, group = index & (LANES - 1), index >> 7
    outs = []
    for at in range(0, index.shape[1], LANES):
        value = jnp.zeros((index.shape[0], LANES), jnp.int32)
        for g in range(table.shape[1] // LANES):
            got = jnp.take_along_axis(
                table[:, g * LANES : (g + 1) * LANES],
                within[:, at : at + LANES],
                axis=1,
                mode="promise_in_bounds",
            )
            value = jnp.where(group[:, at : at + LANES] == g, got, value)
        outs.append(value)
    return outs[0] if len(outs) == 1 else jnp.concatenate(outs, axis=1)


def steps(count, body):
    if count <= 16:
        for i in range(count):
            body(i)
    else:
        def step(i, carry):
            body(i)
            return carry
        lax.fori_loop(0, count, step, 0)


def kernel(
    domains, per_owner,
    tile_hbm, row_hbm, cross_hbm, src_hbm, w_hbm, out_ref,
    tile_ref, row_ref, cross_ref, src_ref,
    wide_tile, wide_row, wide_cross, send_to, link_one, link_two,
    w_ref, pack, buf, acc, edge, beyond, twin_ref, rim_acc, rim_out, rim_in,
    in_sem, w_sem, send_sem, recv_sem, side_sem, wrecv_sem, edge_sem, flag_sem,
    twin_sem, rim_sem,
):
    me = lax.axis_index("dom")
    core = lax.axis_index("tm")
    other = 1 - core
    links, width = w_ref.shape[1], w_ref.shape[3]
    blocks, comps, half, cells = src_ref.shape
    tiles = acc.shape[0]
    link_count = links // tiles
    count = comps * half
    full = per_owner * comps
    planes = full + 1
    mesh_type = pl.DeviceIdType.MESH
    mid, quarter = domains // 2, domains // 4
    upper = me // mid
    lower = 1 - upper
    plane = me // quarter
    inner = (plane + 1) // 2 % 2 * quarter
    even = (1 - plane % 2) * quarter

    def key(d):
        hops = d % 2 + d // 2 % 2 + d // quarter
        shift = (0, 0, -1, 4)
        moved = sum(shift[p] * (d // quarter == p) for p in range(4))
        return (4 * hops + moved) * domains + d

    def wait_if(condition, sem, value):
        @pl.when(condition)
        def _():
            pl.semaphore_wait(sem, value)

    near_from = inner // quarter

    def mailbox(offset):
        return 2 + near_from * (1 + offset)

    inputs = [
        pltpu.make_async_copy(source, target, in_sem.at[i // 3])
        for i, (source, target) in enumerate(
            (
                (tile_hbm, tile_ref),
                (cross_hbm, cross_ref),
                (row_hbm, row_ref),
                (src_hbm, src_ref),
            )
        )
    ]
    for load in inputs:
        load.start()

    barrier = pltpu.get_barrier_semaphore()
    pl.semaphore_signal(barrier, inc=1, device_id=(me, other), device_id_type=mesh_type)


    def greet(i):
        to = domains - 1 - i

        @pl.when(key(to) > key(me))
        def _():
            pl.semaphore_signal(barrier, inc=1, device_id=(to, core), device_id_type=mesh_type)

    steps(domains, greet)

    load_w = pltpu.make_async_copy(w_hbm, w_ref.at[core], w_sem)
    load_w.start()

    wide_tile[...] = jnp.zeros_like(wide_tile)
    wide_cross[...] = jnp.zeros_like(wide_cross)
    wide_row[...] = jnp.zeros_like(wide_row)

    def swap_to(part):
        return pltpu.make_async_remote_copy(
            src_ref=w_hbm,
            dst_ref=w_ref.at[part],
            send_sem=side_sem,
            recv_sem=wrecv_sem,
            device_id=(me, other),
            device_id_type=mesh_type,
        )

    swap = swap_to(core)
    twin = pltpu.make_async_remote_copy(
        src_ref=src_hbm,
        dst_ref=twin_ref,
        send_sem=side_sem,
        recv_sem=twin_sem,
        device_id=(me, other),
        device_id_type=mesh_type,
    )
    gives = (core == 0) & (near_from == 1)
    takes = (core == 1) & (near_from == 1)
    def below(start, number):
        return sum((key(start + i) < key(me)).astype(jnp.int32) for i in range(number))

    before, near_before = below(0, domains), below(upper * mid, mid)

    flag = me % quarter + plane % 2 * (quarter - me % quarter)

    def announce(i):
        to = i

        @pl.when(key(to) < key(me))
        def _():
            box = jnp.where(to // mid == upper, quarter + 1, flag)
            pl.semaphore_signal(
                flag_sem.at[box], inc=1, device_id=(to, core), device_id_type=mesh_type
            )

    for load in inputs[:3]:
        load.wait()
    wide_tile[:, : tile_ref.shape[1]] = jnp.broadcast_to(
        tile_ref[...], (link_count, tile_ref.shape[1])
    )
    wide_cross[:, : cross_ref.shape[1]] = cross_ref[...]
    wide_row[:, : row_ref.shape[1]] = jnp.broadcast_to(
        row_ref[...], (link_count, row_ref.shape[1])
    )
    owners = -(-domains // LANES) * LANES
    around = lax.broadcasted_iota(jnp.int32, (1, owners), 1)
    lane = lax.broadcasted_iota(jnp.int32, (link_count, owners), 1)
    named = lookup(wide_row[...], wide_cross[...])
    rows = []
    for t in range(tiles):
        slot = jnp.minimum(lane * tiles + t, tile_ref.shape[1] - 1)
        rows.append(lookup(named, lookup(wide_tile[...], slot)))

    base = me * blocks
    locals_ = [
        jnp.where((row >= base) & (row < base + blocks), row - base, BIG) for row in rows
    ]
    last = jnp.full((1, owners), -1, jnp.int32)
    for j in range(per_owner):
        left = [jnp.where(at > last, at, BIG) for at in locals_]
        last = jnp.min(functools.reduce(jnp.minimum, left), axis=0, keepdims=True)
        index = jnp.minimum(last, blocks - 1)
        for d in range(domains):
            send_to[d * per_owner + j] = index[0, d]

    def fill(d):
        for j in range(per_owner):
            pack[pl.ds(d * planes + j * comps, comps)] = src_ref[send_to[d * per_owner + j]]

    inputs[3].wait()
    steps(domains, fill)
    for j in range(per_owner):
        buf[pl.ds(me * planes + j * comps, comps)] = src_ref[send_to[me * per_owner + j]]

    def exchange(to, box, start=0, number=full):
        return pltpu.make_async_remote_copy(
            src_ref=pack.at[pl.ds(to * planes + start, number)],
            dst_ref=buf.at[pl.ds(me * planes + start, number)],
            send_sem=send_sem,
            recv_sem=recv_sem.at[box],
            device_id=(to, core),
            device_id_type=mesh_type,
        )

    def across(to, **part):
        exchange(to, mailbox((me ^ to) % quarter), **part).start()

    def first_of(i):
        to = me ^ (domains - 1 - i) ^ even
        return jnp.where(plane == 3, to, lower * mid + i)

    def first(i, **part):
        to = first_of(i)
        wait_if(key(to) > key(me), flag_sem.at[to % quarter], 1)
        across(to, **part)

    def second(i, **part):
        across(me ^ (mid + quarter - 1 - i) ^ even, **part)

    def beside(known):
        def send(i):
            r = mid - 1 - i
            to = me ^ r

            @pl.when((key(to) < key(me)) == known)
            def _():
                exchange(to, r // quarter).start()

        if domains <= 16:
            steps(mid - 1, send)
        else:
            steps(quarter, send)
            steps(quarter - 1, lambda i: send(i + quarter))

    pl.semaphore_wait(barrier, 1 + before)
    steps(domains, announce)
    pl.when(gives)(twin.start)
    swap.start()
    def rim_of(i):
        to, lines = lower * mid + i, []
        for j in range(per_owner):
            block = twin_ref[send_to[to * per_owner + j]].astype(jnp.float32)
            lines.append(block[:, half - 1])
        if half > full:
            lines.append(jnp.zeros((half - full, cells), jnp.float32))
        pack[to * planes + full] = jnp.concatenate(lines, axis=0).astype(jnp.bfloat16)

    def rim_alone(i):
        to = first_of(i)

        @pl.when(to > 0)
        def _():
            across(to, start=full, number=1)

    early = quarter - 1

    def fork(send, start, number):
        @pl.when(takes)
        def _():
            steps(number, lambda i: send(i + start, number=planes))

        @pl.when(jnp.logical_not(takes))
        def _():
            steps(number, lambda i: send(i + start))

    pl.when(upper == 0)(lambda: beside(True))
    steps(early, first)

    @pl.when(takes)
    def _():
        twin.wait_recv()
        steps(mid, rim_of)
        steps(early, rim_alone)

    fork(first, early, quarter - early)

    later = lower * mid + quarter
    due = quarter - below(later, quarter)

    @pl.when(upper == 1)
    def _():
        wait_if(due > 0, flag_sem.at[quarter], due)
        fork(second, 0, quarter)
        beside(True)

    wait_if(near_before < mid - 1, flag_sem.at[quarter + 1], mid - 1 - near_before)
    beside(False)

    @pl.when(upper == 0)
    def _():
        pl.semaphore_wait(flag_sem.at[quarter], due)
        fork(second, 0, quarter)


    link = lax.broadcasted_iota(jnp.int32, (link_count, owners), 0)
    mine = []
    for t in range(tiles):
        column = jnp.sum(jnp.where(lane == me, rows[t], 0), axis=1, keepdims=True)
        at = column - around * blocks
        mine.append(jnp.where((at >= 0) & (at < blocks), at, BIG))
    last = jnp.full((1, owners), -1, jnp.int32)
    for j in range(per_owner):
        least = [jnp.where(at > last, at, BIG) for at in mine]
        last = jnp.min(functools.reduce(jnp.minimum, least), axis=0, keepdims=True)
        one = jnp.full((link_count, owners), BIG, jnp.int32)
        two = jnp.full((link_count, owners), -1, jnp.int32)
        for t in range(tiles):
            hit = (mine[t] == last) & (last < BIG)
            one = jnp.minimum(one, jnp.where(hit, link + t * link_count, BIG))
            two = jnp.maximum(two, jnp.where(hit, link + t * link_count, -1))
        one = jnp.min(one, axis=0, keepdims=True)
        two = jnp.max(two, axis=0, keepdims=True)
        for i in range(domains):
            link_one[i * per_owner + j] = one[0, i]
            link_two[i * per_owner + j] = two[0, i]

    acc[...] = jnp.zeros_like(acc)

    def product(sources, offsets=None):
        rimmed = offsets is not None
        totals = [acc[t] for t in range(tiles)]
        outer = [[0.0] * tiles for _ in range(per_owner)]
        for k, frm in enumerate(sources):
            for j in range(per_owner):
                here = buf[pl.ds(frm * planes + j * comps, comps)].astype(jnp.float32)
                lhs = here.reshape(count, cells)
                if rimmed:
                    rest = rim_in[offsets[k]].astype(jnp.float32)
                    rim = buf[frm * planes + full].astype(jnp.float32)
                    rim = jnp.where(core == 0, rest, jnp.where(me == 0, 0.0, rim))
                    lhs = jnp.concatenate([lhs, rim], axis=0)
                lhs = lhs.astype(jnp.bfloat16)
                one = link_one[frm * per_owner + j]
                two = link_two[frm * per_owner + j]
                at_one, at_two = jnp.minimum(one, links - 1), jnp.maximum(two, 0)
                quad = jnp.concatenate(
                    [w_ref[0, at_one], w_ref[1, at_one], w_ref[0, at_two], w_ref[1, at_two]],
                    axis=1,
                )
                both = jnp.dot(lhs, quad, preferred_element_type=jnp.float32)
                for t in range(tiles):
                    begin, end = t * link_count, (t + 1) * link_count
                    part = jnp.where(
                        (one >= begin) & (one < end), both[:, : 2 * width], 0.0
                    ) + jnp.where((two >= begin) & (two < end), both[:, 2 * width :], 0.0)
                    totals[t] += part[:count]
                    if rimmed:
                        outer[j][t] += part[count:]
        for t in range(tiles):
            acc[t] = totals[t]
            if rimmed:
                parts = [outer[j][t][j * comps : (j + 1) * comps] for j in range(per_owner)]
                rim_acc[t] += sum(parts)

    def arrive(box, number):
        rows_in = buf.at[pl.ds(0, number)]
        pltpu.make_async_remote_copy(
            src_ref=rows_in,
            dst_ref=rows_in,
            send_sem=send_sem,
            recv_sem=recv_sem.at[box],
            device_id=(me, other),
            device_id_type=mesh_type,
        ).wait_recv()

    def beyond_mid(i, apart):
        return me ^ (mid + i) ^ (quarter * apart)

    load_w.wait()
    swap_to(other).wait_recv()

    far, near = 1 - near_from, near_from
    outmost = jnp.where(plane == 0, 1, 0)

    def own_half(i):
        return me ^ (quarter + i)

    def far_half(i):
        return beyond_mid(i, far)

    def near_half(i):
        return beyond_mid(i, near)

    rim_acc[...] = jnp.zeros_like(rim_acc)
    halo = pltpu.make_async_remote_copy(
        src_ref=edge,
        dst_ref=beyond,
        send_sem=side_sem,
        recv_sem=edge_sem,
        device_id=(me, other),
        device_id_type=mesh_type,
    )

    tardy = (core == 0) & (me == 0)

    def give_edge():
        now = acc[...].reshape(tiles, comps, half, 2 * width)
        edge[...] = jnp.where(core == 0, now[:, :, half - 1], now[:, :, 0])
        halo.start()

    if domains <= 16:
        product([me])
        arrive(0, (quarter - 1) * full)
        product([me ^ r for r in range(1, quarter)])
        arrive(1 + outmost, quarter * full)
        product([jnp.where(plane == 0, far_half(i), own_half(i)) for i in range(quarter)])
        arrive(2 - outmost, quarter * full)
        product([jnp.where(plane == 0, own_half(i), far_half(i)) for i in range(quarter)])
        pl.when(jnp.logical_not(tardy))(give_edge)
    else:
        arrive(0, (quarter - 1) * full)
        arrive(1, quarter * full)
        arrive(2, quarter * full)
        steps(mid, lambda r: product([me ^ r]))
        steps(quarter, lambda i: product([far_half(i)]))
        pl.when(jnp.logical_not(tardy))(give_edge)

    bare = (core == 0) | (me == 0)

    def arrive_near(offset):
        @pl.when(bare)
        def _():
            arrive(3 + offset, full)

        @pl.when(jnp.logical_not(bare))
        def _():
            arrive(3 + offset, planes)

    def offset_of(i):
        return quarter - 1 - i

    def handed(base):
        return pltpu.make_async_remote_copy(
            src_ref=rim_out.at[pl.ds(base, 2)],
            dst_ref=rim_in.at[pl.ds(base, 2)],
            send_sem=side_sem,
            recv_sem=rim_sem.at[base // 2],
            device_id=(me, other),
            device_id_type=mesh_type,
        )

    def hand(offset):
        frm, lines = near_half(offset), []
        for j in range(per_owner):
            block = buf[pl.ds(frm * planes + j * comps, comps)].astype(jnp.float32)
            lines.append(block[:, 0])
        if half > full:
            lines.append(jnp.zeros((half - full, cells), jnp.float32))
        rim_out[offset] = jnp.concatenate(lines, axis=0).astype(jnp.bfloat16)

    def late(i):
        pair = [offset_of(i), offset_of(i + 1)]
        base = pair[0] // 2 * 2
        for offset in pair:
            arrive_near(offset)

        @pl.when(core == 1)
        def _():
            for offset in pair:
                hand(offset)
            handed(base).start()

        pl.when(core == 0)(handed(base).wait_recv)
        product([near_half(offset) for offset in pair], pair)

    steps(quarter // 2, lambda i: late(2 * i))
    pl.when(tardy)(give_edge)

    total = acc[...].reshape(tiles, comps, half, 2 * width)

    out_ref[0] = total.astype(jnp.bfloat16)

    def drain(number):
        sent = pack.at[pl.ds(0, number)]
        pltpu.make_async_remote_copy(
            src_ref=sent,
            dst_ref=sent,
            send_sem=send_sem,
            recv_sem=recv_sem.at[0],
            device_id=(me, other),
            device_id_type=mesh_type,
        ).wait_send()

    @pl.when(takes & (plane == 1))
    def _():
        drain((domains - 1) * full + mid)

    @pl.when(takes & (plane == 2))
    def _():
        drain((domains - 1) * full + mid - 1)

    @pl.when(jnp.logical_not(takes))
    def _():
        drain((domains - 1) * full)

    halo.wait_recv()
    sample = lax.broadcasted_iota(jnp.int32, (half, 2 * width), 0)
    for t in range(tiles):
        past = beyond[t] + rim_acc[t]
        for p in range(comps):
            now = total[t, p]
            outer = jnp.broadcast_to(past[p : p + 1], now.shape)
            later = pltpu.roll(now, half - 1, 0)
            prior = pltpu.roll(now, 1, 0)
            later = jnp.where((sample == half - 1) & (core == 0), outer, later)
            prior = jnp.where((sample == 0) & (core == 1), outer, prior)
            rate = jnp.where(
                (sample == 0) & (core == 0),
                later - now,
                jnp.where(
                    (sample == half - 1) & (core == 1), now - prior, (later - prior) * 0.5
                ),
            )
            out_ref[1, t, p] = rate.astype(jnp.bfloat16)
    swap.wait_send()
    pl.when(gives)(twin.wait_send)
    halo.wait_send()

    @pl.when(core == 1)
    def _():
        steps(quarter // 2, lambda i: handed(2 * i).wait_send())


def deliver(both_ref, source_ref, rate_ref, sem):
    copies = [
        pltpu.make_async_copy(both_ref.at[i], out, sem.at[i])
        for i, out in enumerate((source_ref, rate_ref))
    ]
    for copy in copies:
        copy.start()
    for copy in copies:
        copy.wait()


def shards(sources, weights, intersect, block_row, slot_tile):
    domains = lax.axis_size("dom")
    tiles, link_count, cells, width = weights.shape
    blocks, comps, half, _ = sources.shape
    links = tiles * link_count
    pool = links // 2
    per_owner = (pool + domains - 1) // domains
    vmem, smem = pltpu.VMEM, pltpu.SMEM
    shape = (tiles, comps, half, 2 * width)
    out = jax.ShapeDtypeStruct(shape, jnp.bfloat16)
    block = (half, cells)
    planes = per_owner * comps + 1
    dma, regular = pltpu.SemaphoreType.DMA, pltpu.SemaphoreType.REGULAR
    in_vmem = pl.BlockSpec(memory_space=vmem)
    anywhere = pl.BlockSpec(memory_space=pl.ANY)

    def wide(n):
        return vmem((link_count, -(-n // LANES) * LANES), jnp.int32)

    both = pl.pallas_call(
        functools.partial(kernel, domains, per_owner),
        out_shape=vmem((2,) + shape, jnp.bfloat16),
        in_specs=[anywhere] * 5,
        out_specs=in_vmem,
        scratch_shapes=[
            vmem((1, slot_tile.shape[0]), jnp.int32),
            vmem((1, block_row.shape[0]), jnp.int32),
            vmem((link_count, intersect.shape[0]), jnp.int32),
            vmem(sources.shape, jnp.bfloat16),
            wide(slot_tile.shape[0]),
            wide(block_row.shape[0]),
            wide(intersect.shape[0]),
            smem((domains * per_owner,), jnp.int32),
            smem((domains * per_owner,), jnp.int32),
            smem((domains * per_owner,), jnp.int32),
            vmem((2, links, cells, width), jnp.bfloat16),
            vmem((domains * planes,) + block, jnp.bfloat16),
            vmem((domains * planes,) + block, jnp.bfloat16),
            vmem((tiles, comps * half, 2 * width), jnp.float32),
            vmem((tiles, comps, 2 * width), jnp.float32),
            vmem((tiles, comps, 2 * width), jnp.float32),
            vmem(sources.shape, jnp.bfloat16),
            vmem((tiles, comps, 2 * width), jnp.float32),
            vmem((domains // 4,) + block, jnp.bfloat16),
            vmem((domains // 4,) + block, jnp.bfloat16),
            dma((2,)),
            dma,
            dma,
            dma((3 + domains // 4,)),
            dma,
            dma,
            dma,
            regular((domains // 4 + 2,)),
            dma,
            dma((domains // 8,)),
        ],
        compiler_params=pltpu.CompilerParams(
            collective_id=0,
            has_side_effects=True,
        ),
        cost_estimate=pl.CostEstimate(
            flops=4 * comps * half * weights.size,
            bytes_accessed=2 * weights.size,
            transcendentals=0,
        ),
    )(
        slot_tile.reshape(1, -1),
        block_row.reshape(1, -1),
        intersect.T,
        sources,
        weights.reshape(links, cells, width),
    )
    return pl.pallas_call(
        deliver,
        out_shape=(out, out),
        in_specs=[in_vmem],
        out_specs=(anywhere, anywhere),
        scratch_shapes=[dma((2,))],
    )(pltpu.with_memory_space_constraint(both, vmem))


def solution(mesh):
    return jax.shard_map(
        shards,
        mesh=mesh,
        in_specs=(P("dom", None, "tm", None), P("dom", None, None, "tm"), P(), P(), P()),
        out_specs=(P("dom", None, "tm", None), P("dom", None, "tm", None)),
        check_vma=False,
    )
```
